512 devices in a mesh: kgrp: 2 (over y), pw: 64 (over z, core), band: 4 (over x).
Axes of the slice: x: 4, y: 2, z: 32, core: 2. Of those that a mesh axis runs over, the one named last changes fastest.
The devices are a block of a 4x8x32 slice.
Arguments:
- waves: float32 [128, 4, 256, 256], P('band', 'kgrp', 'pw'), parts along dimension 1, as said below
- forward: float32 [128, 4, 256, 256], P('band', 'kgrp', 'pw'), parts along dimension 1, as said below
- backward: float32 [128, 4, 256, 256], P('band', 'kgrp', 'pw'), parts along dimension 1, as said below
- projectors: float32 [256, 2, 256, 256], P('kgrp', None, 'pw'), parts along dimension 0, as said below
- potential: float32 [256, 256], P('pw'), may hold values from 0.25 to 2
- strengths: float32 [128], replicated, may hold values from 0.5 to 4
- shifts: float32 [128], P('band'), may hold values from 0.5 to 2
Outputs:
- response: float32 [128, 4, 256, 256], P('band', 'kgrp', 'pw'), parts along dimension 1
- derivative: float32 [128, 4, 256, 256], P('band', 'kgrp', 'pw'), parts along dimension 1
The draws below stay inside these ranges and needn't reach their ends.
There are 2 independent parts, one for each index of `kgrp`. The reference program is written for one: setup_inputs(seed, part) draws one part's arguments, and reference() takes and returns one part's arrays. A program takes and returns all parts, laid end to end along the dimension named above; an argument that names none is the same for every part. Nothing has to cross between parts.
Inputs may be any that keep to these rules, and one draw needn't show every extreme that they name: `waves`: real and imaginary parts of every band's coefficients are drawn independently at every grid point. `forward`: the margin of the slab's bands with these coefficients is an invertible matrix. `backward`: the margin of the slab's bands with these coefficients is an invertible matrix. `projectors`: real and imaginary parts of every projector are drawn independently at every grid point.
All inputs are finite; a program needn't handle non-finite values.
Results may differ from the reference program's by a relative error of at most 0.0003.
Values sent between devices are 32-bit elements; how exact they have to be, the bound alone decides.
A program may use at most 64 MiB of HBM per device.

```python
import math
import jax
import jax.numpy as jnp
from jax import lax

SLAB = 128
NPROJ = 128
F2 = 256
ITERS = 2
F1 = 256


precise = lax.Precision.HIGHEST


def combine_drawn(vectors, coeffs):
    table = jnp.stack([jnp.stack([coeffs[0], coeffs[1]]), jnp.stack([-coeffs[1], coeffs[0]])])
    return jnp.einsum('ixg,xyij->jyg', vectors, table, precision=precise)


def rough(key, count_rows):
    shape = (count_rows, 2, F1 * F2)
    values = jnp.clip(jax.random.normal(key, shape, jnp.float32), -6.0, 6.0) * 0.70710677
    return values


def neighbour(base, wave_flat, projector_flat):
    mixing = jax.random.normal(jax.random.fold_in(base, 1), (2, SLAB, SLAB), jnp.float32) * (0.2 / math.sqrt(2.0 * SLAB))
    mixing = mixing.at[0].add(jnp.eye(SLAB, dtype=jnp.float32))
    coeffs = jax.random.normal(jax.random.fold_in(base, 2), (2, NPROJ, SLAB), jnp.float32) * (0.70710677 / math.sqrt(NPROJ))
    noise = (rough(jax.random.fold_in(base, 3), SLAB) + combine_drawn(projector_flat, coeffs)) * 0.70710677
    return combine_drawn(wave_flat, mixing) + 0.1 * noise


def joint(key):
    projector_flat = rough(jax.random.fold_in(key, 101), NPROJ)
    wave_flat = rough(jax.random.fold_in(key, 102), SLAB)
    ahead = neighbour(jax.random.fold_in(key, 104), wave_flat, projector_flat)
    behind = neighbour(jax.random.fold_in(key, 105), wave_flat, projector_flat)
    return (wave_flat.reshape(SLAB, 2, F1, F2), ahead.reshape(SLAB, 2, F1, F2), behind.reshape(SLAB, 2, F1, F2), projector_flat.reshape(NPROJ, 2, F1, F2))


def draw_waves(key, part):
    return joint(key)[0]


def draw_forward(key, part):
    return joint(key)[1]


def draw_backward(key, part):
    return joint(key)[2]


def draw_projectors(key, part):
    return joint(key)[3]


def block_levels(own_key, extent, split, least, high):
    def one(position, blocks):
        draws = jax.random.uniform(jax.random.fold_in(jax.random.fold_in(own_key, 6), position), (blocks,), jnp.float32, least / len(split), high / len(split))
        return jnp.repeat(jnp.exp(draws), extent[position] // blocks).reshape((-1,) + (1,) * (len(extent) - position - 1))

    loudness = one(*split[0])
    for cut in split[1:]:
        loudness = loudness * one(*cut)
    return loudness


def setup_inputs(seed: int = 0, part: int = 0) -> dict:
    arg_keys = jax.random.split(jax.random.key(seed), 8)
    own_keys = jax.random.split(jax.random.fold_in(arg_keys[7], part), 8)
    return {
        "waves": draw_waves(jax.random.fold_in(jax.random.fold_in(arg_keys[7], part), 71), part),
        "forward": draw_forward(jax.random.fold_in(jax.random.fold_in(arg_keys[7], part), 71), part),
        "backward": draw_backward(jax.random.fold_in(jax.random.fold_in(arg_keys[7], part), 71), part),
        "projectors": draw_projectors(jax.random.fold_in(jax.random.fold_in(arg_keys[7], part), 71), part),
        "potential": jnp.clip(0.25 + 1.75 * jax.random.uniform(arg_keys[4], (F2, F1), jnp.float32) ** block_levels(arg_keys[4], (F2, F1), ((0, 64),), -0.2, 0.2), 0.25, 2.0),
        "strengths": jnp.clip(jnp.exp(jax.random.uniform(arg_keys[5], (NPROJ,), jnp.float32, math.log(0.5), math.log(4.0))), 0.5, 4.0),
        "shifts": jnp.clip(jnp.exp(math.log(2.0) - 1.3862944 * jax.random.uniform(arg_keys[6], (SLAB,), jnp.float32) ** block_levels(arg_keys[6], (SLAB,), ((0, 4),), -0.2, 0.2)), 0.5, 2.0),
    }


precise = lax.Precision.HIGHEST
string_step = 0.05
kinetic_scale = 4.0

def margin(left_set, right_set):
    products = jnp.einsum('ixg,jyg->xyij', left_set, right_set, precision=precise)
    return jnp.stack([products[0, 0] + products[1, 1], products[0, 1] - products[1, 0]])

def combine(vectors, coeffs):
    table = jnp.stack([jnp.stack([coeffs[0], coeffs[1]]), jnp.stack([-coeffs[1], coeffs[0]])])
    return jnp.einsum('ixg,xyij->jyg', vectors, table, precision=precise)

def invert(matrix):
    real_part = matrix[0]
    imag_part = matrix[1]
    embedded = jnp.concatenate([jnp.concatenate([real_part, -imag_part], 1), jnp.concatenate([imag_part, real_part], 1)], 0)
    normal = jnp.dot(embedded.T, embedded, precision=precise)
    lower_factor = jnp.linalg.cholesky(normal)
    middle = lax.linalg.triangular_solve(lower_factor, embedded.T, left_side=True, lower=True)
    inverse = lax.linalg.triangular_solve(lower_factor, middle, left_side=True, lower=True, transpose_a=True)
    count_rows = real_part.shape[0]
    return jnp.stack([inverse[:count_rows, :count_rows], inverse[count_rows:, :count_rows]])

def centred(index, length):
    shifted = (index + length // 2) % length - length // 2
    return shifted.astype(jnp.float32) / length

def smooth_term(vectors, potential):
    field = lax.complex(vectors[:, 0], vectors[:, 1])
    real_space = jnp.fft.ifft2(field) * potential.T[None]
    returned = jnp.fft.fft2(real_space)
    return jnp.stack([jnp.real(returned), jnp.imag(returned)], axis=1)

def operate(direction, potential, projector_flat, strengths, diagonal):
    count_bands = direction.shape[0]
    points = F1 * F2
    coupling = margin(projector_flat, direction.reshape(count_bands, 2, points)) / points
    nonlocal_part = combine(projector_flat, coupling * strengths[None, :, None]).reshape(direction.shape)
    return diagonal * direction + smooth_term(direction, potential) + nonlocal_part

def reference(waves, forward, backward, projectors, potential, strengths, shifts):
    points = F1 * F2
    waves_flat = waves.reshape(SLAB, 2, points)
    forward_flat = forward.reshape(SLAB, 2, points)
    backward_flat = backward.reshape(SLAB, 2, points)
    forward_margin = margin(waves_flat, forward_flat) / points
    backward_margin = margin(waves_flat, backward_flat) / points
    forward_inverse = invert(forward_margin)
    backward_inverse = invert(backward_margin)
    moved = combine(forward_flat, forward_inverse) - combine(backward_flat, backward_inverse)
    derivative = (moved / (2.0 * string_step)).reshape(SLAB, 2, F1, F2)
    first_index = jnp.arange(F1, dtype=jnp.int32)
    second_index = jnp.arange(F2, dtype=jnp.int32)
    first_freq = centred(first_index, F1)
    second_freq = centred(second_index, F2)
    kinetic = kinetic_scale * (first_freq[:, None] * first_freq[:, None] + second_freq[None, :] * second_freq[None, :])
    diagonal = kinetic[None, None] + shifts[:, None, None, None]
    projector_flat = projectors.reshape(NPROJ, 2, points)
    residual = -derivative
    direction = residual
    solution = jnp.zeros_like(residual)
    norm_now = jnp.sum(residual * residual, axis=(1, 2, 3))
    for turn in range(ITERS):
        image = operate(direction, potential, projector_flat, strengths, diagonal)
        curvature = jnp.sum(direction * image, axis=(1, 2, 3))
        alpha = (norm_now / curvature)[:, None, None, None]
        solution = solution + alpha * direction
        if turn + 1 < ITERS:
            residual = residual - alpha * image
            norm_next = jnp.sum(residual * residual, axis=(1, 2, 3))
            direction = residual + (norm_next / norm_now)[:, None, None, None] * direction
            norm_now = norm_next
    return (solution, derivative)
```

```python
import functools
import math

import jax
import jax.numpy as jnp
import ml_dtypes
import numpy as np
from jax import lax
from jax.experimental import pallas as pl
from jax.experimental.pallas import tpu as pltpu
from jax.sharding import PartitionSpec as P

MESH = pl.DeviceIdType.MESH
HIGHEST = lax.Precision.HIGHEST
string_step = 0.05
kinetic_scale = 4.0
LANES = 128
TILE = 8

NN = (((1,), (0,)), ((), ()))
NT = (((1,), (1,)), ((), ()))


def exact(a, b, dims=NN):
    return lax.dot_general(a, b, dims, precision=HIGHEST, preferred_element_type=jnp.float32)


def single(a, b, dims):
    return lax.dot_general(a, b, dims, preferred_element_type=jnp.float32)


def halves(a):
    high = a.astype(jnp.bfloat16)
    low = (a - high.astype(jnp.float32)).astype(jnp.bfloat16)
    return high, low


def triple(a, b, dims=NN):
    (ah, al), (bh, bl) = a, b
    return single(ah, bh, dims) + (single(ah, bl, dims) + single(al, bh, dims))


def iota(shape, dim):
    return lax.broadcasted_iota(jnp.int32, shape, dim)


def swap_blocks(tiles):
    u = iota(tiles.shape, 1) % 4
    w = iota(tiles.shape, 2) // (LANES // 4)
    turned = pltpu.roll(tiles, LANES // 2, 2)
    below, above = pltpu.roll(turned, TILE - 2, 1), pltpu.roll(turned, 2, 1)
    same, upper = (u // 2) == (w // 2), (u // 2) < (w // 2)
    tiles = jnp.where(same, tiles, jnp.where(upper, below, above))
    below = pltpu.roll(pltpu.roll(tiles, LANES // 4, 2), TILE - 1, 1)
    above = pltpu.roll(pltpu.roll(tiles, LANES - LANES // 4, 2), 1, 1)
    same, upper = (u % 2) == (w % 2), (u % 2) < (w % 2)
    return jnp.where(same, tiles, jnp.where(upper, below, above))


def kernel(
    n, nx, points,
    w_ref, f_ref, b_ref, p_ref, diag_ref, pot_ref, str_ref,
    t2h_ref, t2l_ref, t1h_ref, t1l_ref, t3h_ref, t3l_ref,
    der_ref, sol_ref,
    ph_ref, pl_ref, near, mpart, mrs, mfull, mall, nmat, zmat,
    vec, res, img,
    sendb, recvb, sendc, recvc, sende, recve,
    cpart, crs, cfull, cpart2, crs2,
    scal, scals, scal2, scals2, field_ref,
    xs, xr, ms, mr, cs, cr, es, er,
):
    me = lax.axis_index("pw")
    mx = lax.axis_index("band")
    bands = w_ref.shape[0] // 4
    half = w_ref.shape[1] // 2
    every = nx * bands
    right, left = lax.rem(mx + 1, nx), lax.rem(mx + nx - 1, nx)

    def other(i):
        part = (i + 1) // 2
        return lax.rem(me + n // 2 + part * (2 * lax.rem(i, 2) - 1) + n, n)

    barrier = pltpu.get_barrier_semaphore()

    def greet(i, carry):
        pl.semaphore_signal(barrier, inc=1, device_id={"pw": other(i)}, device_id_type=MESH)
        return carry

    lax.fori_loop(0, n - 1, greet, 0)
    for step in range(1, nx):
        pl.semaphore_signal(
            barrier, inc=1, device_id={"band": lax.rem(mx + step, nx)}, device_id_type=MESH
        )
    pl.semaphore_wait(barrier, n - 1 + nx - 1)

    def remote(src, dst, send, recv, axis, target):
        return pltpu.make_async_remote_copy(
            src_ref=src, dst_ref=dst, send_sem=send, recv_sem=recv,
            device_id={axis: target}, device_id_type=MESH,
        )

    def exchange(src, dst, send, recv):
        dst[pl.ds(me, 1)] = src[pl.ds(me, 1)]

        def one(i, carry):
            t = other(i)
            remote(src.at[t], dst.at[me], send, recv, "pw", t).start()
            return carry

        lax.fori_loop(0, n - 1, one, 0)

    def tell(src, dst, send, recv):
        def one(i, carry):
            remote(src, dst, send, recv, "pw", other(i)).start()
            return carry

        lax.fori_loop(0, n - 1, one, 0)

    def arrived(dst, count, recv):
        some = dst.at[pl.ds(0, count)]
        remote(some, some, recv, recv, "pw", other(0)).wait_recv()

    def left_here(src, count, send):
        some = src.at[pl.ds(0, count)]
        remote(some, some, send, send, "pw", other(0)).wait_send()

    def to_owners(src, dst, send, recv):
        tiles = src.shape[0]
        stride = n // tiles

        def one(i, carry):
            t = lax.rem(i + me // stride, tiles)
            owner = t * stride

            @pl.when(owner != me)
            def _():
                remote(src.at[t], dst.at[me], send, recv, "pw", owner).start()

            @pl.when(owner == me)
            def _():
                dst[pl.ds(me, 1)] = src[pl.ds(t, 1)]

            return carry

        lax.fori_loop(0, tiles, one, 0)

    def sent_to_owners(src, send):
        tiles = src.shape[0]
        owns = lax.rem(me, n // tiles) == 0

        @pl.when(owns)
        def _():
            left_here(src, tiles - 1, send)

        @pl.when(jnp.logical_not(owns))
        def _():
            left_here(src, tiles, send)

    def owners_tell(buf, full, recv, tell_send, tell_recv):
        tiles = full.shape[0]
        stride = n // tiles

        @pl.when(lax.rem(me, stride) == 0)
        def _():
            arrived(buf, n - 1, recv)
            t = me // stride
            full[pl.ds(t, 1)] = jnp.sum(buf[...], axis=0, keepdims=True)
            tell(full.at[t], full.at[t], tell_send, tell_recv)

    def told(full, recv):
        tiles = full.shape[0]
        owns = lax.rem(me, n // tiles) == 0

        @pl.when(owns)
        def _():
            arrived(full, tiles - 1, recv)

        @pl.when(jnp.logical_not(owns))
        def _():
            arrived(full, tiles, recv)

    def owners_done(buf, full, send):
        tiles = full.shape[0]

        @pl.when(lax.rem(me, n // tiles) == 0)
        def _():
            left_here(buf, n - 1, send)

    near[0, 0] = f_ref[...]
    near[0, 1] = b_ref[...]
    to_right = [
        remote(f_ref, near.at[3, 0], xs.at[0], xr.at[0], "band", right),
        remote(b_ref, near.at[3, 1], xs.at[1], xr.at[1], "band", right),
    ]
    to_left = [
        remote(b_ref, near.at[1, 1], xs.at[2], xr.at[2], "band", left),
        remote(f_ref, near.at[1, 0], xs.at[3], xr.at[3], "band", left),
    ]
    for a, b in zip(to_right, to_left):
        a.start()
        b.start()

    ph_ref[...], pl_ref[...] = halves(p_ref[...])
    own = []
    for r in range(4):
        rows = w_ref[r * bands : (r + 1) * bands, :]
        own.append(jnp.concatenate([rows, jnp.concatenate([-rows[:, half:], rows[:, :half]], 1)], 0))

    def margin_of(slot, which):
        total = None
        for r in range(4):
            term = exact(own[r], near[slot, which, r * bands : (r + 1) * bands, :], NT)
            total = term if total is None else total + term
        mpart_rows = pl.ds(which * 2 * bands, 2 * bands)
        nmat[0, 0, mpart_rows, slot * bands : (slot + 1) * bands] = total

    margin_of(0, 0)
    margin_of(0, 1)
    to_right[0].wait_recv()
    far_right = remote(near.at[3, 0], near.at[2, 0], xs.at[4], xr.at[4], "band", right)
    far_right.start()
    to_left[0].wait_recv()
    far_left = remote(near.at[1, 1], near.at[2, 1], xs.at[5], xr.at[5], "band", left)
    far_left.start()
    margin_of(3, 0)
    margin_of(1, 1)
    to_right[1].wait_recv()
    to_left[1].wait_recv()
    margin_of(3, 1)
    margin_of(1, 0)
    far_right.wait_recv()
    margin_of(2, 0)
    far_left.wait_recv()
    margin_of(2, 1)
    turned = pltpu.roll(nmat[0, 0], mx * bands, 1)
    mpart[...] = turned.reshape(mpart.shape)

    to_owners(mpart, mrs, ms.at[0], mr.at[0])
    owners_tell(mrs, mfull, mr.at[0], ms.at[1], mr.at[1])
    told(mfull, mr.at[1])
    mall[pl.ds(mx, 1)] = mfull[...][None]
    for step in range(1, nx):
        t = lax.rem(mx + step, nx)
        remote(mfull, mall.at[mx], ms.at[2], mr.at[2], "band", t).start()
    some = mall.at[pl.ds(0, nx - 1)]
    across = remote(some, some, ms.at[2], mr.at[2], "band", right)
    across.wait_recv()

    def margin_full(which, part):
        tiles_each = bands // TILE
        at = (which * 2 + part) * tiles_each
        rows = [mall[x, at : at + tiles_each].reshape(bands, every) for x in range(nx)]
        return jnp.concatenate(rows, 0) / points

    for which in range(2):
        real, imag = margin_full(which, 0), margin_full(which, 1)
        nmat[which, 0] = exact(real, real, NT) + exact(imag, imag, NT)
        nmat[which, 1] = exact(real, imag, NT) - exact(imag, real, NT)

    def eliminate(c, carry):
        lane = iota((every, every), 1)
        row = iota((every, every), 0)
        on_lane, on_row = lane == c, row == c
        at = jnp.full((every, every), 0, jnp.int32) + c
        for which in range(2):
            real, imag = nmat[which, 0], nmat[which, 1]
            row_r = nmat[which, 0, pl.ds(c, 1), :]
            row_i = nmat[which, 1, pl.ds(c, 1), :]
            col_r = jnp.take_along_axis(real, at, axis=1)
            col_i = jnp.take_along_axis(imag, at, axis=1)
            pivot = jnp.sum(jnp.where(lane[:1] == c, row_r, 0.0), axis=1, keepdims=True)
            scale = 1.0 / pivot
            row_r = jnp.where(lane[:1] == c, 1.0, row_r) * scale
            row_i = jnp.where(lane[:1] == c, 0.0, row_i) * scale
            real = jnp.where(on_lane, 0.0, real) - (col_r * row_r - col_i * row_i)
            imag = jnp.where(on_lane, 0.0, imag) - (col_r * row_i + col_i * row_r)
            nmat[which, 0] = jnp.where(on_row, row_r, real)
            nmat[which, 1] = jnp.where(on_row, row_i, imag)
        return carry

    lax.fori_loop(0, every, eliminate, 0)

    for which in range(2):
        real, imag = margin_full(which, 0), margin_full(which, 1)
        mine = pl.ds(pl.multiple_of(mx * bands, TILE), bands)
        nr, ni = nmat[which, 0, mine, :], nmat[which, 1, mine, :]
        zr = exact(nr, real) + exact(ni, imag)
        zi = exact(ni, real) - exact(nr, imag)
        both = pltpu.roll(jnp.concatenate([zr, zi], 0), lax.rem((nx - mx) * bands, every), 1)
        zmat[:, which * every : (which + 1) * every] = both if which == 0 else -both

    coeff = zmat[...]
    for r in range(4):
        rows = slice(r * bands, (r + 1) * bands)
        blocks = [near[d, which, rows, :] for which in range(2) for d in range(nx)]
        mixed = exact(coeff, jnp.concatenate(blocks, 0))
        dr = (mixed[:bands, :half] - mixed[bands:, half:]) / (2.0 * string_step)
        di = (mixed[:bands, half:] + mixed[bands:, :half]) / (2.0 * string_step)
        der_ref[rows, :half] = dr
        der_ref[rows, half:] = di
        vec[rows, :half] = -dr
        vec[rows, half:] = -di

    def forth(src, send, recv, sem):
        parts = halves(src[...])
        out = triple((t2h_ref[...], t2l_ref[...]), parts, NT)
        send[...] = swap_blocks(out.reshape(n, TILE, LANES))
        exchange(send, recv, es.at[sem], er.at[sem])

    def fields(recv, sem):
        arrived(recv, n - 1, er.at[sem])
        parts = halves(recv[...].reshape(n * TILE, LANES))
        return triple((t1h_ref[...], t1l_ref[...]), parts)

    def project(src, part, buf, send, recv):
        total = None
        for r in range(4):
            rows = src[r * bands : (r + 1) * bands, :]
            both = jnp.concatenate([rows, jnp.concatenate([rows[:, half:], -rows[:, :half]], 1)], 0)
            at = slice(r * every, (r + 1) * every)
            term = triple(halves(both), (ph_ref[at, :], pl_ref[at, :]), NT)
            total = term if total is None else total + term
        part[...] = (total / points).reshape(part.shape)
        to_owners(part, buf, send, recv)

    def per_band(values):
        return sum(values[r * bands : (r + 1) * bands] for r in range(1, 4)) + values[:bands]

    def summed(values):
        return per_band(jnp.sum(values, axis=1, keepdims=True))

    def as_row(column, first):
        shape = (column.shape[0], LANES)
        chosen = iota(shape, 1) == iota(shape, 0) + first
        return jnp.sum(jnp.where(chosen, column, 0.0), axis=0, keepdims=True)

    def as_column(row, first):
        shape = (bands, LANES)
        chosen = iota(shape, 1) == iota(shape, 0) + first
        return jnp.sum(jnp.where(chosen, row, 0.0), axis=1, keepdims=True)

    def lanes_per_band(row, first):
        row = row + pltpu.roll(row, LANES // 2, 1)
        row = row + pltpu.roll(row, LANES // 4, 1)
        lane = iota(row.shape, 1)
        return jnp.where((lane >= first) & (lane < first + bands), row, 0.0)

    def down_rows(column):
        return jnp.concatenate([column] * 4, 0)

    diag = jnp.concatenate([diag_ref[...]] * 2, 1)
    stren = str_ref[...]

    forth(vec, sendb, recvb, 0)
    project(vec, cpart, crs, cs.at[0], cr.at[0])
    d = vec[...]
    scal_row = as_row(summed(diag * d * d), 0) + as_row(summed(d * d), 2 * bands)
    owners_tell(crs, cfull, cr.at[0], cs.at[1], cr.at[1])
    field = fields(recvb, 0)
    field_ref[...] = field
    pot = jnp.concatenate([pot_ref[...]] * 2, 0)
    weighted = field * pot
    energy = jnp.sum(weighted * field, axis=0, keepdims=True)
    sendc[...] = triple((t3h_ref[...], t3l_ref[...]), halves(weighted)).reshape(sendc.shape)
    scal[...] = scal_row + lanes_per_band(energy, 0)
    tell(scal, scals.at[me], es.at[3], er.at[3])
    exchange(sendc, recvc, es.at[1], er.at[1])
    scals[pl.ds(me, 1)] = scal[...][None]

    told(cfull, cr.at[1])
    coupled = cfull[...].reshape(2 * bands, every)
    weights = halves(coupled * stren)
    for r in range(4):
        at = slice(r * every, (r + 1) * every)
        rows = slice(r * bands, (r + 1) * bands)
        mixed = triple(weights, (ph_ref[at, :], pl_ref[at, :]))
        img[rows, :half] = mixed[:bands, :half] - mixed[bands:, half:]
        img[rows, half:] = mixed[:bands, half:] + mixed[bands:, :half]
    pair = jnp.sum(stren * coupled * coupled, axis=1, keepdims=True)
    own_pair = points * (pair[:bands] + pair[bands:])
    arrived(scals, n - 1, er.at[3])
    totals = jnp.sum(scals[...], axis=0)
    norm_now = as_column(totals, 2 * bands)
    curvature = as_column(totals, 0) + own_pair
    alpha = norm_now / curvature

    arrived(recvc, n - 1, er.at[1])
    back = swap_blocks(recvc[...]).reshape(n * TILE, LANES).T
    smooth = triple(halves(back), (t2h_ref[...], t2l_ref[...]))
    d = vec[...]
    image = diag * d + smooth + img[...]
    res[...] = d - down_rows(alpha) * image

    forth(res, sende, recve, 2)
    project(res, cpart2, crs2, cs.at[2], cr.at[2])
    d, r2 = vec[...], res[...]
    stiff = diag * r2
    row2 = as_row(summed(stiff * r2), 0) + as_row(summed(stiff * d), bands)
    row2 = row2 + as_row(summed(r2 * r2), 2 * bands)
    scal2[...] = row2
    tiles2 = cpart2.shape[0]
    stride2 = n // tiles2

    @pl.when(lax.rem(me, stride2) == 0)
    def _():
        arrived(crs2, n - 1, cr.at[2])
        t = me // stride2
        mine = jnp.sum(crs2[...], axis=0)
        old = cfull[pl.ds(t, 1)].reshape(TILE, every)
        first = lax.rem(t * TILE, bands)
        with_mine = points * jnp.sum(stren * mine * mine, axis=1, keepdims=True)
        with_old = points * jnp.sum(stren * mine * old, axis=1, keepdims=True)
        scal2[...] = scal2[...] + as_row(with_mine, first) + as_row(with_old, first + bands)

    field2 = fields(recve, 2)
    weighted2 = field2 * jnp.concatenate([pot_ref[...]] * 2, 0)
    own2 = jnp.sum(weighted2 * field2, axis=0, keepdims=True)
    cross2 = jnp.sum(weighted2 * field_ref[...], axis=0, keepdims=True)
    scal2[...] = scal2[...] + lanes_per_band(own2, 0) + lanes_per_band(cross2, bands)
    tell(scal2, scals2.at[me], es.at[4], er.at[4])
    scals2[pl.ds(me, 1)] = scal2[...][None]
    arrived(scals2, n - 1, er.at[4])
    totals2 = jnp.sum(scals2[...], axis=0)
    norm_next = as_column(totals2, 2 * bands)
    beta = norm_next / norm_now
    curvature2 = (
        as_column(totals2, 0) + 2.0 * beta * as_column(totals2, bands) + beta * beta * curvature
    )
    alpha2 = norm_next / curvature2
    sol_ref[...] = down_rows(alpha + alpha2 * beta) * vec[...] + down_rows(alpha2) * res[...]

    for copy in to_right + to_left + [far_right, far_left]:
        copy.wait_send()
    across.wait_send()
    sent_to_owners(mpart, ms.at[0])
    owners_done(mrs, mfull, ms.at[1])
    sent_to_owners(cpart, cs.at[0])
    owners_done(crs, cfull, cs.at[1])
    sent_to_owners(cpart2, cs.at[2])
    left_here(sendb, n - 1, es.at[0])
    left_here(sendc, n - 1, es.at[1])
    left_here(sende, n - 1, es.at[2])
    left_here(scals, n - 1, es.at[3])
    left_here(scals2, n - 1, es.at[4])


def centred(index, length):
    shifted = (index + length // 2) % length - length // 2
    return shifted.astype(jnp.float32) / length


def split_table(table):
    table = table.astype(np.float32)
    high = table.astype(ml_dtypes.bfloat16)
    low = (table - high.astype(np.float32)).astype(ml_dtypes.bfloat16)
    return high, low


def tables(length, peers):
    index = np.arange(length)
    angle = (index[:, None] * index[None, :] % length) * (2.0 * math.pi / length)
    cosine, sine = np.cos(angle) / math.sqrt(length), np.sin(angle) / math.sqrt(length)
    out = np.block([[cosine, -sine], [sine, cosine]])
    order = np.arange(2 * length).reshape(2, peers, length // peers).transpose(1, 0, 2).reshape(-1)
    first, third = out[order], out.T[order]
    return (*split_table(first), *split_table(third.T.copy()), *split_table(third))


def flat(array):
    items, parts, rows, width = array.shape
    return array.transpose(2, 0, 1, 3).reshape(rows * items, parts * width)


def body(n, nx, waves, forward, backward, projectors, potential, strengths, shifts):
    bands, parts, rows, width = waves.shape
    length = rows * n
    points = float(length * width)
    every = nx * bands
    count = projectors.shape[0]
    first_index = lax.axis_index("pw") * rows + jnp.arange(rows, dtype=jnp.int32)
    second_index = jnp.arange(width, dtype=jnp.int32)
    first_freq, second_freq = centred(first_index, length), centred(second_index, width)
    kinetic = kinetic_scale * (
        first_freq[:, None] * first_freq[:, None] + second_freq[None, :] * second_freq[None, :]
    )
    diag = (kinetic[:, None, :] + shifts[None, :, None]).reshape(rows * bands, width)
    pot = jnp.repeat(potential.T, bands, axis=1)
    shape = (rows * bands, parts * width)
    f32 = functools.partial(pltpu.VMEM, dtype=jnp.float32)
    full, tiles = (n, TILE, LANES), 2 * bands // TILE
    vmem = pl.BlockSpec(memory_space=pltpu.VMEM)
    dma = pltpu.SemaphoreType.DMA
    der, sol = pl.pallas_call(
        functools.partial(kernel, n, nx, points),
        out_shape=[jax.ShapeDtypeStruct(shape, jnp.float32)] * 2,
        in_specs=[vmem] * 13,
        out_specs=[vmem] * 2,
        scratch_shapes=[
            pltpu.VMEM((rows * count, parts * width), jnp.bfloat16),
            pltpu.VMEM((rows * count, parts * width), jnp.bfloat16),
            f32((nx, 2, *shape)),
            f32((2 * tiles, TILE, LANES)), f32(full), f32((2 * tiles, TILE, LANES)),
            f32((nx, 2 * tiles, TILE, LANES)), f32((2, 2, every, every)), f32((2 * bands, 2 * every)),
            f32(shape), f32(shape), f32(shape),
            f32(full), f32(full), f32(full), f32(full), f32(full), f32(full),
            f32((tiles, TILE, LANES)), f32(full), f32((tiles, TILE, LANES)),
            f32((tiles, TILE, LANES)), f32(full),
            f32((1, LANES)), f32((n, 1, LANES)), f32((1, LANES)), f32((n, 1, LANES)),
            f32((n * TILE, LANES)),
            dma((6,)), dma((6,)), dma((3,)), dma((3,)), dma((3,)), dma((3,)), dma((5,)), dma((5,)),
        ],
        compiler_params=pltpu.CompilerParams(
            collective_id=0, has_side_effects=True, vmem_limit_bytes=60 * 1024 * 1024
        ),
    )(
        flat(waves), flat(forward), flat(backward), flat(projectors), diag, pot,
        strengths.reshape(1, count), *[jnp.asarray(t) for t in tables(length, n)],
    )

    def unflat(array):
        return array.reshape(rows, bands, parts, width).transpose(1, 2, 0, 3)

    return unflat(sol), unflat(der)


def solution(mesh):
    bands = P("band", "kgrp", "pw", None)
    return jax.shard_map(
        functools.partial(body, mesh.shape["pw"], mesh.shape["band"]),
        mesh=mesh,
        in_specs=(bands, bands, bands, P("kgrp", None, "pw", None), P("pw", None), P(), P("band")),
        out_specs=(bands, bands),
        check_vma=False,
    )
```

```python
import functools
import math

import jax
import jax.numpy as jnp
import ml_dtypes
import numpy as np
from jax import lax
from jax.experimental import pallas as pl
from jax.experimental.pallas import tpu as pltpu
from jax.sharding import PartitionSpec as P

MESH = pl.DeviceIdType.MESH
HIGHEST = lax.Precision.HIGHEST
string_step = 0.05
kinetic_scale = 4.0
LANES = 128
TILE = 8

NN = (((1,), (0,)), ((), ()))
NT = (((1,), (1,)), ((), ()))


def exact(a, b, dims=NN):
    return lax.dot_general(a, b, dims, precision=HIGHEST, preferred_element_type=jnp.float32)


def single(a, b, dims):
    return lax.dot_general(a, b, dims, preferred_element_type=jnp.float32)


def halves(a):
    high = a.astype(jnp.bfloat16)
    low = (a - high.astype(jnp.float32)).astype(jnp.bfloat16)
    return high, low


def triple(a, b, dims=NN):
    (ah, al), (bh, bl) = a, b
    return single(ah, bh, dims) + (single(ah, bl, dims) + single(al, bh, dims))


def iota(shape, dim):
    return lax.broadcasted_iota(jnp.int32, shape, dim)


def swap_blocks(tiles):
    u = iota(tiles.shape, 1) % 4
    w = iota(tiles.shape, 2) // (LANES // 4)
    turned = pltpu.roll(tiles, LANES // 2, 2)
    below, above = pltpu.roll(turned, TILE - 2, 1), pltpu.roll(turned, 2, 1)
    same, upper = (u // 2) == (w // 2), (u // 2) < (w // 2)
    tiles = jnp.where(same, tiles, jnp.where(upper, below, above))
    below = pltpu.roll(pltpu.roll(tiles, LANES // 4, 2), TILE - 1, 1)
    above = pltpu.roll(pltpu.roll(tiles, LANES - LANES // 4, 2), 1, 1)
    same, upper = (u % 2) == (w % 2), (u % 2) < (w % 2)
    return jnp.where(same, tiles, jnp.where(upper, below, above))


def kernel(
    n, nx, points,
    w_raw, f_raw, b_raw, p_ref, shift_ref, pot_ref, str_ref,
    t2h_ref, t2l_ref,
    der_raw, sol_raw,
    w_ref, f_ref, b_ref,
    diag_ref, pots_ref, ph_ref, pl_ref, t1h_ref, t1l_ref, t3h_ref, t3l_ref, wide, qt, near, mpart, mrs, mfull, mall, nmat, zmat,
    vec, res, img,
    sendb, recvb, sendc, recvc, sende, recve,
    cpart, crs, cfull, cpart2, crs2,
    scal, scals, scal2, scals2, field_ref,
    known, xs, xr, ms, mr, cs, cr, es, er,
):
    me = lax.axis_index("pw")
    mx = lax.axis_index("band")
    bands = w_ref.shape[0] // 4
    half = w_ref.shape[1] // 2
    every = nx * bands
    right, left = lax.rem(mx + 1, nx), lax.rem(mx + nx - 1, nx)

    def other(i):
        part = (i + 1) // 2
        return lax.rem(me + n // 2 + part * (2 * lax.rem(i, 2) - 1) + n, n)


    def flatten(raw, flat_ref):
        for r in range(4):
            for part in range(2):
                lanes = slice(part * half, (part + 1) * half)
                flat_ref[r * bands : (r + 1) * bands, lanes] = raw[:, part, r, :]

    barrier = pltpu.get_barrier_semaphore()

    def at_distance(d):
        return lax.rem(me + d + n, n)

    def greet(d, axis="pw", base=None):
        target = at_distance(d) if base is None else base
        pl.semaphore_signal(barrier, inc=1, device_id={axis: target}, device_id_type=MESH)

    partner = me + 1 - 2 * lax.rem(me, 2)
    greet(0, "pw", partner)
    greet(2)
    greet(-2)
    for step in range(1, nx):
        greet(0, "band", lax.rem(mx + step, nx))
    flatten(w_raw, w_ref)
    flatten(f_raw, f_ref)
    flatten(b_raw, b_ref)
    pl.semaphore_wait(barrier, 3 + nx - 1)

    def learn(k):
        d = 2 << k
        for target in (at_distance(d), at_distance(-d)):
            pl.semaphore_signal(known.at[k], inc=1, device_id={"pw": target}, device_id_type=MESH)
        pl.semaphore_wait(known.at[k], 2)

    rounds = (n // 4).bit_length() - 1

    def learn_partner():
        pl.semaphore_signal(known.at[rounds], inc=1, device_id={"pw": partner}, device_id_type=MESH)
        pl.semaphore_wait(known.at[rounds], 1)

    def remote(src, dst, send, recv, axis, target):
        return pltpu.make_async_remote_copy(
            src_ref=src, dst_ref=dst, send_sem=send, recv_sem=recv,
            device_id={axis: target}, device_id_type=MESH,
        )

    group = max(k for k in (1, 3, 7, 9) if (n - 1) % k == 0)

    def to_others(start):
        def some(i, carry):
            for k in range(group):
                start(other(i * group + k))
            return carry

        lax.fori_loop(0, (n - 1) // group, some, 0)

    def exchange(src, dst, send, recv):
        dst[pl.ds(me, 1)] = src[pl.ds(me, 1)]
        to_others(lambda t: remote(src.at[t], dst.at[me], send, recv, "pw", t).start())

    def tell(src, dst, send, recv):
        to_others(lambda t: remote(src, dst, send, recv, "pw", t).start())

    def arrived(dst, count, recv):
        some = dst.at[pl.ds(0, count)]
        remote(some, some, recv, recv, "pw", other(0)).wait_recv()

    def left_here(src, count, send):
        some = src.at[pl.ds(0, count)]
        remote(some, some, send, send, "pw", other(0)).wait_send()

    def to_owners(src, dst, send, recv):
        tiles = src.shape[0]
        stride = n // tiles

        def one(i, carry):
            t = lax.rem(i + me // stride, tiles)
            owner = t * stride

            @pl.when(owner != me)
            def _():
                remote(src.at[t], dst.at[me], send, recv, "pw", owner).start()

            @pl.when(owner == me)
            def _():
                dst[pl.ds(me, 1)] = src[pl.ds(t, 1)]

            return carry

        lax.fori_loop(0, tiles, one, 0)

    def sent_to_owners(src, send):
        tiles = src.shape[0]
        owns = lax.rem(me, n // tiles) == 0

        @pl.when(owns)
        def _():
            left_here(src, tiles - 1, send)

        @pl.when(jnp.logical_not(owns))
        def _():
            left_here(src, tiles, send)

    def owners_tell(buf, full, recv, tell_send, tell_recv):
        tiles = full.shape[0]
        stride = n // tiles

        @pl.when(lax.rem(me, stride) == 0)
        def _():
            arrived(buf, n - 1, recv)
            t = me // stride
            full[pl.ds(t, 1)] = jnp.sum(buf[...], axis=0, keepdims=True)
            tell(full.at[t], full.at[t], tell_send, tell_recv)

    def told(full, recv):
        tiles = full.shape[0]
        owns = lax.rem(me, n // tiles) == 0

        @pl.when(owns)
        def _():
            arrived(full, tiles - 1, recv)

        @pl.when(jnp.logical_not(owns))
        def _():
            arrived(full, tiles, recv)

    def owners_done(buf, full, send):
        tiles = full.shape[0]

        @pl.when(lax.rem(me, n // tiles) == 0)
        def _():
            left_here(buf, n - 1, send)

    part_rows = w_ref.shape[0] // 2
    lower, upper = pl.ds(0, part_rows), pl.ds(part_rows, part_rows)

    def over_band(src, dst, at, target):
        return remote(src, dst, xs.at[at], xr.at[at], "band", target)

    to_right = [
        over_band(w_ref.at[lower], wide.at[3, lower], 0, right),
        over_band(w_ref.at[upper], wide.at[3, upper], 1, right),
        over_band(f_ref, near.at[3, 0], 6, right),
        over_band(b_ref, near.at[3, 1], 8, right),
    ]
    to_left = [
        over_band(w_ref.at[upper], wide.at[1, upper], 2, left),
        over_band(w_ref.at[lower], wide.at[1, lower], 3, left),
        over_band(b_ref, near.at[1, 1], 9, left),
        over_band(f_ref, near.at[1, 0], 7, left),
    ]
    for a, b in zip(to_right, to_left):
        a.start()
        b.start()
    wide[0] = w_ref[...]
    near[0, 0] = f_ref[...]
    near[0, 1] = b_ref[...]
    learn(0)
    learn(1)

    own = []
    for r in range(4):
        both = []
        for src in (f_ref, b_ref):
            rows = src[r * bands : (r + 1) * bands, :]
            both += [rows, jnp.concatenate([rows[:, half:], -rows[:, :half]], 1)]
        own.append(halves(jnp.concatenate(both, 0)))

    def margin_of(slot):
        total = None
        for r in range(4):
            term = triple(own[r], halves(wide[slot, r * bands : (r + 1) * bands, :]), NT)
            total = term if total is None else total + term
        nmat[0, 0, :, slot * bands : (slot + 1) * bands] = total

    to_right[0].wait_recv()
    far_right = over_band(wide.at[3, lower], wide.at[2, lower], 4, right)
    far_right.start()
    to_left[0].wait_recv()
    far_left = over_band(wide.at[1, upper], wide.at[2, upper], 5, left)
    far_left.start()
    learn(2)
    margin_of(0)
    to_right[1].wait_recv()
    margin_of(3)
    to_left[1].wait_recv()
    margin_of(1)
    for k in range(3, rounds):
        learn(k)
    learn_partner()
    far_right.wait_recv()
    far_left.wait_recv()
    margin_of(2)
    turned = pltpu.roll(nmat[0, 0], mx * bands, 1)
    mpart[...] = turned.reshape(mpart.shape)

    to_owners(mpart, mrs, ms.at[0], mr.at[0])
    for r in range(4):
        for part in range(2):
            rows = slice(r * every, (r + 1) * every)
            lanes = slice(part * half, (part + 1) * half)
            ph_ref[rows, lanes], pl_ref[rows, lanes] = halves(p_ref[:, part, r, :])
    u = me * 4 + iota((4 * bands, half), 0) // bands
    w = iota((4 * bands, half), 1)
    u, w = centred(u, 4 * n), centred(w, half)
    diag_ref[...] = kinetic_scale * (u * u + w * w) + shift_ref[...]
    columns = jnp.concatenate([pot_ref[...]] * 2, 0).T
    at = iota((4 * n, LANES), 1) // bands
    spread = jnp.zeros((4 * n, LANES), jnp.float32)
    for k in range(4):
        spread = jnp.where(at == k, columns[:, k : k + 1], spread)
    pots_ref[...] = spread
    shape = t2h_ref.shape
    row_part, lane_part = iota(shape, 0) % TILE // (TILE // 2), iota(shape, 1) // half
    flip = jnp.where(row_part == lane_part, 1.0, -1.0)
    inverse_table = (t2h_ref[...].astype(jnp.float32) + t2l_ref[...].astype(jnp.float32)) * flip
    t3h_ref[...], t3l_ref[...] = halves(inverse_table)
    t1h_ref[...], t1l_ref[...] = halves(inverse_table.T)
    owners_tell(mrs, mfull, mr.at[0], ms.at[1], mr.at[1])
    to_right[2].wait_recv()
    far_f = over_band(near.at[3, 0], near.at[2, 0], 10, right)
    far_f.start()
    to_left[2].wait_recv()
    far_b = over_band(near.at[1, 1], near.at[2, 1], 11, left)
    far_b.start()
    told(mfull, mr.at[1])
    mall[pl.ds(mx, 1)] = mfull[...][None]
    for step in range(1, nx):
        t = lax.rem(mx + step, nx)
        remote(mfull, mall.at[mx], ms.at[2], mr.at[2], "band", t).start()
    some = mall.at[pl.ds(0, nx - 1)]
    across = remote(some, some, ms.at[2], mr.at[2], "band", right)
    across.wait_recv()

    def margin_full(which, part):
        tiles_each = bands // TILE
        at = (which * 2 + part) * tiles_each
        rows = [mall[x, at : at + tiles_each].reshape(bands, every) for x in range(nx)]
        return jnp.concatenate(rows, 0) / points

    for which in range(2):
        real, imag = margin_full(which, 0), margin_full(which, 1)
        nmat[which, 0] = exact(real, real, NT) + exact(imag, imag, NT)
        nmat[which, 1] = exact(imag, real, NT) - exact(real, imag, NT)
        qt[which, 0] = real.T
        qt[which, 1] = imag.T

    def eliminate(step, carry):
        c = 2 * step
        lane = iota((every, every), 1)
        at_0 = jnp.full((every, every), 0, jnp.int32) + c
        line = iota((1, every), 1)
        for which in range(2):
            real, imag = nmat[which, 0], nmat[which, 1]
            row_r = [nmat[which, 0, pl.ds(c + k, 1), :] for k in range(2)]
            row_i = [nmat[which, 1, pl.ds(c + k, 1), :] for k in range(2)]

            def element(row, k):
                return jnp.sum(jnp.where(line == c + k, row, 0.0), axis=1, keepdims=True)

            first, last = element(row_r[0], 0), element(row_r[1], 1)
            across_r, across_i = element(row_r[0], 1), element(row_i[0], 1)
            scale = 1.0 / (first * last - across_r * across_r - across_i * across_i)
            first, last = first * scale, last * scale
            across_r, across_i = across_r * scale, across_i * scale
            row_r = [jnp.where((line == c) | (line == c + 1), jnp.where(line == c + k, 1.0, 0.0), row_r[k]) for k in range(2)]
            row_i = [jnp.where((line == c) | (line == c + 1), 0.0, row_i[k]) for k in range(2)]
            new_r = [
                last * row_r[0] - across_r * row_r[1] + across_i * row_i[1],
                first * row_r[1] - across_r * row_r[0] - across_i * row_i[0],
            ]
            new_i = [
                last * row_i[0] - across_r * row_i[1] - across_i * row_r[1],
                first * row_i[1] - across_r * row_i[0] + across_i * row_r[0],
            ]
            on = (lane == c) | (lane == c + 1)
            sum_r, sum_i = jnp.where(on, 0.0, real), jnp.where(on, 0.0, imag)
            for k in range(2):
                col_r = jnp.take_along_axis(real, at_0 + k, axis=1)
                col_i = jnp.take_along_axis(imag, at_0 + k, axis=1)
                sum_r = sum_r - (col_r * new_r[k] - col_i * new_i[k])
                sum_i = sum_i - (col_r * new_i[k] + col_i * new_r[k])
            nmat[which, 0] = sum_r
            nmat[which, 1] = sum_i
            for k in range(2):
                nmat[which, 0, pl.ds(c + k, 1), :] = new_r[k]
                nmat[which, 1, pl.ds(c + k, 1), :] = new_i[k]
        return carry

    lax.fori_loop(0, every // 2, eliminate, 0)

    for which in range(2):
        mine = pl.ds(pl.multiple_of(mx * bands, TILE), bands)
        qr, qi = qt[which, 0, mine, :], qt[which, 1, mine, :]
        nr, ni = nmat[which, 0], nmat[which, 1]
        zr = exact(qr, nr) + exact(qi, ni)
        zi = exact(qr, ni) - exact(qi, nr)
        both = pltpu.roll(jnp.concatenate([zr, zi], 0), lax.rem((nx - mx) * bands, every), 1)
        zmat[:, which * every : (which + 1) * every] = both if which == 0 else -both

    to_right[3].wait_recv()
    to_left[3].wait_recv()
    far_f.wait_recv()
    far_b.wait_recv()
    coeff = zmat[...]
    for r in range(4):
        rows = slice(r * bands, (r + 1) * bands)
        blocks = [near[d, which, rows, :] for which in range(2) for d in range(nx)]
        mixed = exact(coeff, jnp.concatenate(blocks, 0))
        dr = (mixed[:bands, :half] - mixed[bands:, half:]) / (2.0 * string_step)
        di = (mixed[:bands, half:] + mixed[bands:, :half]) / (2.0 * string_step)
        der_raw[:, 0, r, :] = dr
        der_raw[:, 1, r, :] = di
        vec[rows, :half] = -dr
        vec[rows, half:] = -di

    def forth(src, send, recv, sem):
        parts = halves(src[...])
        out = triple((t2h_ref[...], t2l_ref[...]), parts, NT)
        send[...] = swap_blocks(out.reshape(n, TILE, LANES))
        exchange(send, recv, es.at[sem], er.at[sem])

    def fields(recv, sem):
        arrived(recv, n - 1, er.at[sem])
        parts = halves(recv[...].reshape(n * TILE, LANES))
        return triple((t1h_ref[...], t1l_ref[...]), parts)

    def project(src, part, buf, send, recv):
        total = None
        for r in range(4):
            rows = src[r * bands : (r + 1) * bands, :]
            both = jnp.concatenate([rows, jnp.concatenate([rows[:, half:], -rows[:, :half]], 1)], 0)
            at = slice(r * every, (r + 1) * every)
            term = triple(halves(both), (ph_ref[at, :], pl_ref[at, :]), NT)
            total = term if total is None else total + term
        part[...] = (total / points).reshape(part.shape)
        to_owners(part, buf, send, recv)

    def per_band(values):
        return sum(values[r * bands : (r + 1) * bands] for r in range(1, 4)) + values[:bands]

    def summed(values):
        return per_band(jnp.sum(values, axis=1, keepdims=True))

    def as_row(column, first):
        shape = (column.shape[0], LANES)
        chosen = iota(shape, 1) == iota(shape, 0) + first
        return jnp.sum(jnp.where(chosen, column, 0.0), axis=0, keepdims=True)

    def as_column(row, first):
        shape = (bands, LANES)
        chosen = iota(shape, 1) == iota(shape, 0) + first
        return jnp.sum(jnp.where(chosen, row, 0.0), axis=1, keepdims=True)

    def lanes_per_band(row, first):
        row = row + pltpu.roll(row, LANES // 2, 1)
        row = row + pltpu.roll(row, LANES // 4, 1)
        lane = iota(row.shape, 1)
        return jnp.where((lane >= first) & (lane < first + bands), row, 0.0)

    def down_rows(column):
        return jnp.concatenate([column] * 4, 0)

    diag = jnp.concatenate([diag_ref[...]] * 2, 1)
    stren = str_ref[...]

    forth(vec, sendb, recvb, 0)
    project(vec, cpart, crs, cs.at[0], cr.at[0])
    d = vec[...]
    scal_row = as_row(summed(diag * d * d), 0) + as_row(summed(d * d), 2 * bands)
    owners_tell(crs, cfull, cr.at[0], cs.at[1], cr.at[1])
    field = fields(recvb, 0)
    field_ref[...] = field
    pot = jnp.concatenate([pots_ref[...]] * 2, 0)
    weighted = field * pot
    energy = jnp.sum(weighted * field, axis=0, keepdims=True)
    sendc[...] = triple((t3h_ref[...], t3l_ref[...]), halves(weighted)).reshape(sendc.shape)
    scal[...] = scal_row + lanes_per_band(energy, 0)
    tell(scal, scals.at[me], es.at[3], er.at[3])
    exchange(sendc, recvc, es.at[1], er.at[1])
    scals[pl.ds(me, 1)] = scal[...][None]

    told(cfull, cr.at[1])
    coupled = cfull[...].reshape(2 * bands, every)
    weights = halves(coupled * stren)
    for r in range(4):
        at = slice(r * every, (r + 1) * every)
        rows = slice(r * bands, (r + 1) * bands)
        mixed = triple(weights, (ph_ref[at, :], pl_ref[at, :]))
        img[rows, :half] = mixed[:bands, :half] - mixed[bands:, half:]
        img[rows, half:] = mixed[:bands, half:] + mixed[bands:, :half]
    pair = jnp.sum(stren * coupled * coupled, axis=1, keepdims=True)
    own_pair = points * (pair[:bands] + pair[bands:])
    arrived(scals, n - 1, er.at[3])
    totals = jnp.sum(scals[...], axis=0)
    norm_now = as_column(totals, 2 * bands)
    curvature = as_column(totals, 0) + own_pair
    alpha = norm_now / curvature

    arrived(recvc, n - 1, er.at[1])
    back = swap_blocks(recvc[...]).reshape(n * TILE, LANES).T
    smooth = triple(halves(back), (t2h_ref[...], t2l_ref[...]))
    d = vec[...]
    image = diag * d + smooth + img[...]
    res[...] = d - down_rows(alpha) * image

    forth(res, sende, recve, 2)
    project(res, cpart2, crs2, cs.at[2], cr.at[2])
    d, r2 = vec[...], res[...]
    stiff = diag * r2
    row2 = as_row(summed(stiff * r2), 0) + as_row(summed(stiff * d), bands)
    row2 = row2 + as_row(summed(r2 * r2), 2 * bands)
    scal2[...] = row2
    tiles2 = cpart2.shape[0]
    stride2 = n // tiles2

    @pl.when(lax.rem(me, stride2) == 0)
    def _():
        arrived(crs2, n - 1, cr.at[2])
        t = me // stride2
        mine = jnp.sum(crs2[...], axis=0)
        old = cfull[pl.ds(t, 1)].reshape(TILE, every)
        first = lax.rem(t * TILE, bands)
        with_mine = points * jnp.sum(stren * mine * mine, axis=1, keepdims=True)
        with_old = points * jnp.sum(stren * mine * old, axis=1, keepdims=True)
        scal2[...] = scal2[...] + as_row(with_mine, first) + as_row(with_old, first + bands)

    field2 = fields(recve, 2)
    weighted2 = field2 * jnp.concatenate([pots_ref[...]] * 2, 0)
    own2 = jnp.sum(weighted2 * field2, axis=0, keepdims=True)
    cross2 = jnp.sum(weighted2 * field_ref[...], axis=0, keepdims=True)
    scal2[...] = scal2[...] + lanes_per_band(own2, 0) + lanes_per_band(cross2, bands)
    tell(scal2, scals2.at[me], es.at[4], er.at[4])
    scals2[pl.ds(me, 1)] = scal2[...][None]
    arrived(scals2, n - 1, er.at[4])
    totals2 = jnp.sum(scals2[...], axis=0)
    norm_next = as_column(totals2, 2 * bands)
    beta = norm_next / norm_now
    curvature2 = (
        as_column(totals2, 0) + 2.0 * beta * as_column(totals2, bands) + beta * beta * curvature
    )
    alpha2 = norm_next / curvature2
    of_first = alpha + alpha2 * beta
    for r in range(4):
        rows = slice(r * bands, (r + 1) * bands)
        total = of_first * vec[rows, :] + alpha2 * res[rows, :]
        for part in range(2):
            sol_raw[:, part, r, :] = total[:, part * half : (part + 1) * half]

    for copy in to_right + to_left + [far_right, far_left, far_f, far_b]:
        copy.wait_send()
    across.wait_send()
    sent_to_owners(mpart, ms.at[0])
    owners_done(mrs, mfull, ms.at[1])
    sent_to_owners(cpart, cs.at[0])
    owners_done(crs, cfull, cs.at[1])
    sent_to_owners(cpart2, cs.at[2])
    left_here(sendb, n - 1, es.at[0])
    left_here(sendc, n - 1, es.at[1])
    left_here(sende, n - 1, es.at[2])
    left_here(scals, n - 1, es.at[3])
    left_here(scals2, n - 1, es.at[4])


def centred(index, length):
    shifted = (index + length // 2) % length - length // 2
    return shifted.astype(jnp.float32) / length


def split_table(table):
    table = table.astype(np.float32)
    high = table.astype(ml_dtypes.bfloat16)
    low = (table - high.astype(np.float32)).astype(ml_dtypes.bfloat16)
    return high, low


def tables(length, peers):
    index = np.arange(length)
    angle = (index[:, None] * index[None, :] % length) * (2.0 * math.pi / length)
    cosine, sine = np.cos(angle) / math.sqrt(length), np.sin(angle) / math.sqrt(length)
    out = np.block([[cosine, -sine], [sine, cosine]])
    order = np.arange(2 * length).reshape(2, peers, length // peers).transpose(1, 0, 2).reshape(-1)
    return split_table(out[order])


def body(n, nx, waves, forward, backward, projectors, potential, strengths, shifts):
    bands, parts, rows, width = waves.shape
    length = rows * n
    points = float(length * width)
    every = nx * bands
    count = projectors.shape[0]
    shape = (rows * bands, parts * width)
    f32 = functools.partial(pltpu.VMEM, dtype=jnp.float32)
    full, tiles = (n, TILE, LANES), 2 * bands // TILE
    vmem = pl.BlockSpec(memory_space=pltpu.VMEM)
    dma = pltpu.SemaphoreType.DMA
    der, sol = pl.pallas_call(
        functools.partial(kernel, n, nx, points),
        out_shape=[jax.ShapeDtypeStruct(waves.shape, jnp.float32)] * 2,
        in_specs=[vmem] * 9,
        out_specs=[vmem] * 2,
        scratch_shapes=[
            f32(shape), f32(shape), f32(shape),
            f32((rows * bands, width)), f32((length, LANES)),
            *[pltpu.VMEM((rows * count, parts * width), jnp.bfloat16)] * 2,
            *[pltpu.VMEM((2 * length, 2 * length), jnp.bfloat16)] * 4,
            f32((nx, *shape)), f32((2, 2, every, every)),
            f32((nx, 2, *shape)),
            f32((2 * tiles, TILE, LANES)), f32(full), f32((2 * tiles, TILE, LANES)),
            f32((nx, 2 * tiles, TILE, LANES)), f32((2, 2, every, every)), f32((2 * bands, 2 * every)),
            f32(shape), f32(shape), f32(shape),
            f32(full), f32(full), f32(full), f32(full), f32(full), f32(full),
            f32((tiles, TILE, LANES)), f32(full), f32((tiles, TILE, LANES)),
            f32((tiles, TILE, LANES)), f32(full),
            f32((1, LANES)), f32((n, 1, LANES)), f32((1, LANES)), f32((n, 1, LANES)),
            f32((n * TILE, LANES)),
            pltpu.SemaphoreType.REGULAR((n.bit_length(),)),
            dma((12,)), dma((12,)), dma((3,)), dma((3,)), dma((3,)), dma((3,)), dma((5,)), dma((5,)),
        ],
        compiler_params=pltpu.CompilerParams(
            collective_id=0, has_side_effects=True, vmem_limit_bytes=60 * 1024 * 1024
        ),
    )(
        waves, forward, backward, projectors, jnp.tile(shifts, rows).reshape(-1, 1), potential,
        strengths.reshape(1, count), *[jnp.asarray(t) for t in tables(length, n)],
    )

    return sol, der


def solution(mesh):
    bands = P("band", "kgrp", "pw", None)
    return jax.shard_map(
        functools.partial(body, mesh.shape["pw"], mesh.shape["band"]),
        mesh=mesh,
        in_specs=(bands, bands, bands, P("kgrp", None, "pw", None), P("pw", None), P(), P("band")),
        out_specs=(bands, bands),
        check_vma=False,
    )
```

```python
import functools
import math

import jax
import jax.numpy as jnp
import ml_dtypes
import numpy as np
from jax import lax
from jax.experimental import pallas as pl
from jax.experimental.pallas import tpu as pltpu
from jax.sharding import PartitionSpec as P

MESH = pl.DeviceIdType.MESH
HIGHEST = lax.Precision.HIGHEST
string_step = 0.05
kinetic_scale = 4.0
LANES = 128
TILE = 8

NN = (((1,), (0,)), ((), ()))
NT = (((1,), (1,)), ((), ()))


def exact(a, b, dims=NN):
    return lax.dot_general(a, b, dims, precision=HIGHEST, preferred_element_type=jnp.float32)


def single(a, b, dims):
    return lax.dot_general(a, b, dims, preferred_element_type=jnp.float32)


def halves(a):
    high = a.astype(jnp.bfloat16)
    low = (a - high.astype(jnp.float32)).astype(jnp.bfloat16)
    return high, low


def triple(a, b, dims=NN):
    (ah, al), (bh, bl) = a, b
    return single(ah, bh, dims) + (single(ah, bl, dims) + single(al, bh, dims))


def iota(shape, dim):
    return lax.broadcasted_iota(jnp.int32, shape, dim)


def swap_blocks(tiles):
    u = iota(tiles.shape, 1) % 4
    w = iota(tiles.shape, 2) // (LANES // 4)
    turned = pltpu.roll(tiles, LANES // 2, 2)
    below, above = pltpu.roll(turned, TILE - 2, 1), pltpu.roll(turned, 2, 1)
    same, upper = (u // 2) == (w // 2), (u // 2) < (w // 2)
    tiles = jnp.where(same, tiles, jnp.where(upper, below, above))
    below = pltpu.roll(pltpu.roll(tiles, LANES // 4, 2), TILE - 1, 1)
    above = pltpu.roll(pltpu.roll(tiles, LANES - LANES // 4, 2), 1, 1)
    same, upper = (u % 2) == (w % 2), (u % 2) < (w % 2)
    return jnp.where(same, tiles, jnp.where(upper, below, above))


def kernel(
    n, nx, points,
    w_raw, f_raw, b_raw, p_ref, shift_ref, pot_ref, str_ref,
    t2h_ref, t2l_ref,
    der_raw, sol_raw,
    w_ref, f_ref, b_ref,
    diag_ref, pots_ref, ph_ref, pl_ref, t1h_ref, t1l_ref, t3h_ref, t3l_ref, wide, qt, near, mpart, mpair, msum, mrs, mfull, mall, nmat, zmat,
    vec, res, img,
    sendb, recvb, sendc, recvc, sende, recve,
    cpart, cpair, csum, crs, cfull, cpart2, cpair2, csum2, crs2,
    scal, spair, scals, scal2, spair2, scals2, field_ref,
    known, xs, xr, zs, zr_sem, ms, mr, mm, cm, cm2, sm, sm2, es, er,
):
    me = lax.axis_index("pw")
    mx = lax.axis_index("band")
    bands = w_ref.shape[0] // 4
    half = w_ref.shape[1] // 2
    every = nx * bands
    right, left = lax.rem(mx + 1, nx), lax.rem(mx + nx - 1, nx)

    def other(i):
        part = (i + 1) // 2
        return lax.rem(me + n // 2 + part * (2 * lax.rem(i, 2) - 1) + n, n)


    def flatten(raw, flat_ref):
        for r in range(4):
            for part in range(2):
                lanes = slice(part * half, (part + 1) * half)
                flat_ref[r * bands : (r + 1) * bands, lanes] = raw[:, part, r, :]

    barrier = pltpu.get_barrier_semaphore()

    partner = me + 1 - 2 * lax.rem(me, 2)

    def at_distance(d):
        return lax.rem(me + d + n, n)

    def greet(d, axis="pw", base=None):
        target = at_distance(d) if base is None else base
        pl.semaphore_signal(barrier, inc=1, device_id={axis: target}, device_id_type=MESH)

    greet(0, "pw", partner)
    greet(2)
    greet(-2)
    for step in range(1, nx):
        greet(0, "band", lax.rem(mx + step, nx))
    flatten(w_raw, w_ref)
    flatten(f_raw, f_ref)
    flatten(b_raw, b_ref)
    pl.semaphore_wait(barrier, 3 + nx - 1)

    def learn(k):
        d = 2 << k
        for target in (at_distance(d), at_distance(-d)):
            pl.semaphore_signal(known.at[k], inc=1, device_id={"pw": target}, device_id_type=MESH)
        pl.semaphore_wait(known.at[k], 2)

    rounds = (n // 4).bit_length() - 1

    def learn_partner():
        pl.semaphore_signal(known.at[rounds], inc=1, device_id={"pw": partner}, device_id_type=MESH)
        pl.semaphore_wait(known.at[rounds], 1)

    def remote(src, dst, send, recv, axis, target):
        return pltpu.make_async_remote_copy(
            src_ref=src, dst_ref=dst, send_sem=send, recv_sem=recv,
            device_id={axis: target}, device_id_type=MESH,
        )

    group = max(k for k in (1, 3, 7, 9) if (n - 1) % k == 0)

    def to_others(start):
        def some(i, carry):
            for k in range(group):
                start(other(i * group + k))
            return carry

        lax.fori_loop(0, (n - 1) // group, some, 0)

    def exchange(src, dst, send, recv):
        dst[pl.ds(me, 1)] = src[pl.ds(me, 1)]
        to_others(lambda t: remote(src.at[t], dst.at[me], send, recv, "pw", t).start())

    core, place, chips = lax.rem(me, 2), me // 2, n // 2

    def line_other(i):
        part = (i + 1) // 2
        chip = lax.rem(place + chips // 2 + part * (2 * lax.rem(i, 2) - 1) + chips, chips)
        return 2 * chip + core

    def tell_line(src, dst, send, recv):
        def one(i, carry):
            remote(src, dst, send, recv, "pw", line_other(i)).start()
            return carry

        lax.fori_loop(0, chips - 1, one, 0)

    def arrived(dst, count, recv):
        some = dst.at[pl.ds(0, count)]
        remote(some, some, recv, recv, "pw", partner).wait_recv()

    def left_here(src, count, send):
        some = src.at[pl.ds(0, count)]
        remote(some, some, send, send, "pw", partner).wait_send()

    def owner_of(tiles):
        stride = chips // (tiles // 2)
        return lax.rem(place, stride) == 0, core * (tiles // 2) + place // stride

    def to_owners(part, pair, summed_pair, dst, sem):
        tiles = part.shape[0] // 2
        stride = chips // tiles
        theirs = pl.ds((1 - core) * tiles, tiles)
        copy = remote(part.at[theirs], pair, sem.at[0], sem.at[1], "pw", partner)
        copy.start()
        copy.wait_recv()
        summed_pair[...] = part[pl.ds(core * tiles, tiles)] + pair[...]

        def one(i, carry):
            t = lax.rem(i + place // stride, tiles)
            owner = 2 * t * stride + core

            @pl.when(owner != me)
            def _():
                remote(
                    summed_pair.at[t], dst.at[place], sem.at[2], sem.at[3], "pw", owner
                ).start()

            @pl.when(owner == me)
            def _():
                dst[pl.ds(place, 1)] = summed_pair[pl.ds(t, 1)]

            return carry

        lax.fori_loop(0, tiles, one, 0)

    def sent_to_owners(part, summed_pair, sem):
        tiles = summed_pair.shape[0]
        owns, _ = owner_of(2 * tiles)
        left_here(part, tiles, sem.at[0])

        @pl.when(owns)
        def _():
            left_here(summed_pair, tiles - 1, sem.at[2])

        @pl.when(jnp.logical_not(owns))
        def _():
            left_here(summed_pair, tiles, sem.at[2])

    def owners_tell(buf, full, sem):
        owns, t = owner_of(full.shape[0])

        @pl.when(owns)
        def _():
            arrived(buf, chips - 1, sem.at[3])
            full[pl.ds(t, 1)] = jnp.sum(buf[...], axis=0, keepdims=True)
            tell_line(full.at[t], full.at[t], sem.at[4], sem.at[5])

    def told(full, sem):
        tiles = full.shape[0] // 2
        owns, _ = owner_of(2 * tiles)

        @pl.when(owns)
        def _():
            arrived(full, tiles - 1, sem.at[5])

        @pl.when(jnp.logical_not(owns))
        def _():
            arrived(full, tiles, sem.at[5])

        mine = full.at[pl.ds(core * tiles, tiles)]
        remote(mine, mine, sem.at[6], sem.at[7], "pw", partner).start()
        arrived(full, tiles, sem.at[7])

    def owners_done(buf, full, sem):
        owns, _ = owner_of(full.shape[0])
        left_here(full, full.shape[0] // 2, sem.at[6])

        @pl.when(owns)
        def _():
            left_here(buf, chips - 1, sem.at[4])

    def add_up(mine, pair, rows, sem):
        remote(mine.at[0], pair, sem.at[0], sem.at[1], "pw", partner).start()
        remote(mine.at[0], pair, sem.at[0], sem.at[1], "pw", partner).wait_recv()
        mine[1] = mine[0] + pair[...]
        tell_line(mine.at[1], rows.at[place], sem.at[2], sem.at[3])
        rows[pl.ds(place, 1)] = mine[1][None]

    def added_up(rows, sem):
        arrived(rows, chips - 1, sem.at[3])
        return jnp.sum(rows[...], axis=0)

    def adding_done(mine, rows, sem):
        remote(mine.at[0], mine.at[0], sem.at[0], sem.at[0], "pw", partner).wait_send()
        left_here(rows, chips - 1, sem.at[2])

    part_rows = w_ref.shape[0] // 2
    lower, upper = pl.ds(0, part_rows), pl.ds(part_rows, part_rows)

    def over_band(src, dst, at, target):
        return remote(src, dst, xs.at[at], xr.at[at], "band", target)

    to_right = [
        over_band(w_ref.at[lower], wide.at[3, lower], 0, right),
        over_band(w_ref.at[upper], wide.at[3, upper], 1, right),
        over_band(f_ref, near.at[3, 0], 6, right),
        over_band(b_ref, near.at[3, 1], 8, right),
    ]
    to_left = [
        over_band(w_ref.at[upper], wide.at[1, upper], 2, left),
        over_band(w_ref.at[lower], wide.at[1, lower], 3, left),
        over_band(b_ref, near.at[1, 1], 9, left),
        over_band(f_ref, near.at[1, 0], 7, left),
    ]
    for a, b in zip(to_right, to_left):
        a.start()
        b.start()
    wide[0] = w_ref[...]
    near[0, 0] = f_ref[...]
    near[0, 1] = b_ref[...]
    learn(0)
    learn(1)

    own = []
    for r in range(4):
        both = []
        for src in (f_ref, b_ref):
            rows = src[r * bands : (r + 1) * bands, :]
            both += [rows, jnp.concatenate([rows[:, half:], -rows[:, :half]], 1)]
        own.append(halves(jnp.concatenate(both, 0)))

    def margin_of(slot):
        total = None
        for r in range(4):
            term = triple(own[r], halves(wide[slot, r * bands : (r + 1) * bands, :]), NT)
            total = term if total is None else total + term
        nmat[0, :, slot * bands : (slot + 1) * bands] = total

    to_right[0].wait_recv()
    far_right = over_band(wide.at[3, lower], wide.at[2, lower], 4, right)
    far_right.start()
    to_left[0].wait_recv()
    far_left = over_band(wide.at[1, upper], wide.at[2, upper], 5, left)
    far_left.start()
    learn(2)
    margin_of(0)
    to_right[1].wait_recv()
    margin_of(3)
    to_left[1].wait_recv()
    margin_of(1)
    for k in range(3, rounds):
        learn(k)
    learn_partner()
    far_right.wait_recv()
    far_left.wait_recv()
    margin_of(2)
    turned = pltpu.roll(nmat[0], mx * bands, 1)
    mpart[...] = turned.reshape(mpart.shape)

    to_owners(mpart, mpair, msum, mrs, mm)
    for r in range(4):
        for part in range(2):
            rows = slice(r * every, (r + 1) * every)
            lanes = slice(part * half, (part + 1) * half)
            ph_ref[rows, lanes], pl_ref[rows, lanes] = halves(p_ref[:, part, r, :])
    u = me * 4 + iota((4 * bands, half), 0) // bands
    w = iota((4 * bands, half), 1)
    u, w = centred(u, 4 * n), centred(w, half)
    diag_ref[...] = kinetic_scale * (u * u + w * w) + shift_ref[...]
    columns = jnp.concatenate([pot_ref[...]] * 2, 0).T
    at = iota((4 * n, LANES), 1) // bands
    spread = jnp.zeros((4 * n, LANES), jnp.float32)
    for k in range(4):
        spread = jnp.where(at == k, columns[:, k : k + 1], spread)
    pots_ref[...] = spread
    shape = t2h_ref.shape
    row_part, lane_part = iota(shape, 0) % TILE // (TILE // 2), iota(shape, 1) // half
    flip = jnp.where(row_part == lane_part, 1.0, -1.0)
    inverse_table = (t2h_ref[...].astype(jnp.float32) + t2l_ref[...].astype(jnp.float32)) * flip
    t3h_ref[...], t3l_ref[...] = halves(inverse_table)
    t1h_ref[...], t1l_ref[...] = halves(inverse_table.T)
    owners_tell(mrs, mfull, mm)
    to_right[2].wait_recv()
    far_f = over_band(near.at[3, 0], near.at[2, 0], 10, right)
    far_f.start()
    to_left[2].wait_recv()
    far_b = over_band(near.at[1, 1], near.at[2, 1], 11, left)
    far_b.start()
    told(mfull, mm)
    mall[pl.ds(mx, 1)] = mfull[...][None]
    for step in range(1, nx):
        t = lax.rem(mx + step, nx)
        remote(mfull, mall.at[mx], ms, mr, "band", t).start()
    some = mall.at[pl.ds(0, nx - 1)]
    across = remote(some, some, ms, mr, "band", right)
    across.wait_recv()

    def margin_full(part):
        tiles_each = bands // TILE
        at = pl.ds((core * 2 + part) * tiles_each, tiles_each)
        rows = [mall[x, at].reshape(bands, every) for x in range(nx)]
        return jnp.concatenate(rows, 0) / points

    real, imag = margin_full(0), margin_full(1)
    nmat[0] = exact(real, real, NT) + exact(imag, imag, NT)
    nmat[1] = exact(imag, real, NT) - exact(real, imag, NT)
    qt[0] = real.T
    qt[1] = imag.T

    def times(a, b):
        return a[0] * b[0] - a[1] * b[1], a[0] * b[1] + a[1] * b[0]

    def minus(a, b):
        return a[0] - b[0], a[1] - b[1]

    def conj(a):
        return a[0], -a[1]

    def solver(first, last, across):
        scale = 1.0 / (first * last - across[0] * across[0] - across[1] * across[1])
        first, last = first * scale, last * scale
        across = (across[0] * scale, across[1] * scale)

        def solve(x, y):
            new_x = minus((last * x[0], last * x[1]), times(across, y))
            return new_x, minus((first * y[0], first * y[1]), times(conj(across), x))

        return solve

    def eliminate(step, carry):
        c = 4 * step
        lane = iota((every, every), 1)
        at_0 = jnp.full((every, every), 0, jnp.int32) + c
        line = iota((1, every), 1)
        lows, highs = (line == c) | (line == c + 1), (line == c + 2) | (line == c + 3)
        on = (lane >= c) & (lane < c + 4)

        def without(row, where):
            return jnp.where(where, 0.0, row[0]), jnp.where(where, 0.0, row[1])

        def unit(row, where, k):
            return jnp.where(where, jnp.where(line == c + k, 1.0, 0.0), row[0]), jnp.where(where, 0.0, row[1])

        real, imag = nmat[0], nmat[1]
        rows = [
            (nmat[0, pl.ds(c + k, 1), :], nmat[1, pl.ds(c + k, 1), :])
            for k in range(4)
        ]

        def one(row, k):
            return jnp.sum(jnp.where(line == c + k, row, 0.0), axis=1, keepdims=True)

        def element(j, k):
            return one(rows[j][0], k), one(rows[j][1], k)

        diag4 = [one(rows[k][0], k) for k in range(4)]
        off = {(j, k): element(j, k) for j in range(4) for k in range(j + 1, 4)}
        solve = solver(diag4[0], diag4[1], off[0, 1])
        head = {k: solve(off[0, k], off[1, k]) for k in (2, 3)}

        def rest(j, k, value):
            value = minus(value, times(conj(off[0, j]), head[k][0]))
            return minus(value, times(conj(off[1, j]), head[k][1]))

        zero = jnp.zeros_like(diag4[2])
        last_solve = solver(
            rest(2, 2, (diag4[2], zero))[0], rest(3, 3, (diag4[3], zero))[0], rest(2, 3, off[2, 3])
        )
        new = list(solve(unit(rows[0], lows, 0), unit(rows[1], lows, 1)))
        tail = []
        for k in (2, 3):
            row = minus(without(rows[k], lows), times(conj(off[0, k]), new[0]))
            row = minus(row, times(conj(off[1, k]), new[1]))
            tail.append(unit(row, highs, k))
        tail = last_solve(*tail)
        for k in range(2):
            row = minus(without(new[k], highs), times(head[2][k], tail[0]))
            new[k] = minus(row, times(head[3][k], tail[1]))
        new += tail
        total = jnp.where(on, 0.0, real), jnp.where(on, 0.0, imag)
        for k in range(4):
            column = (
                jnp.take_along_axis(real, at_0 + k, axis=1),
                jnp.take_along_axis(imag, at_0 + k, axis=1),
            )
            total = minus(total, times(column, new[k]))
        nmat[0], nmat[1] = total
        for k in range(4):
            nmat[0, pl.ds(c + k, 1), :] = new[k][0]
            nmat[1, pl.ds(c + k, 1), :] = new[k][1]
        return carry

    lax.fori_loop(0, every // 4, eliminate, 0)

    mine = pl.ds(pl.multiple_of(mx * bands, TILE), bands)
    qr, qi = qt[0, mine, :], qt[1, mine, :]
    nr, ni = nmat[0], nmat[1]
    zr = exact(qr, nr) + exact(qi, ni)
    zi = exact(qr, ni) - exact(qi, nr)
    both = pltpu.roll(jnp.concatenate([zr, zi], 0), lax.rem((nx - mx) * bands, every), 1)
    zmat[pl.ds(core, 1)] = jnp.where(core == 0, both, -both)[None]
    swap = remote(zmat.at[core], zmat.at[core], zs, zr_sem, "pw", partner)
    swap.start()

    to_right[3].wait_recv()
    to_left[3].wait_recv()
    far_f.wait_recv()
    far_b.wait_recv()
    swap.wait_recv()
    coeff = jnp.concatenate([zmat[0], zmat[1]], 1)
    for r in range(4):
        rows = slice(r * bands, (r + 1) * bands)
        blocks = [near[d, which, rows, :] for which in range(2) for d in range(nx)]
        mixed = exact(coeff, jnp.concatenate(blocks, 0))
        dr = (mixed[:bands, :half] - mixed[bands:, half:]) / (2.0 * string_step)
        di = (mixed[:bands, half:] + mixed[bands:, :half]) / (2.0 * string_step)
        der_raw[:, 0, r, :] = dr
        der_raw[:, 1, r, :] = di
        vec[rows, :half] = -dr
        vec[rows, half:] = -di

    def forth(src, send, recv, sem):
        parts = halves(src[...])
        out = triple((t2h_ref[...], t2l_ref[...]), parts, NT)
        send[...] = swap_blocks(out.reshape(n, TILE, LANES))
        exchange(send, recv, es.at[sem], er.at[sem])

    def fields(recv, sem):
        arrived(recv, n - 1, er.at[sem])
        parts = halves(recv[...].reshape(n * TILE, LANES))
        return triple((t1h_ref[...], t1l_ref[...]), parts)

    def project(src, part, pair, summed_pair, buf, sem):
        total = None
        for r in range(4):
            rows = src[r * bands : (r + 1) * bands, :]
            both = jnp.concatenate([rows, jnp.concatenate([rows[:, half:], -rows[:, :half]], 1)], 0)
            at = slice(r * every, (r + 1) * every)
            term = triple(halves(both), (ph_ref[at, :], pl_ref[at, :]), NT)
            total = term if total is None else total + term
        part[...] = (total / points).reshape(part.shape)
        to_owners(part, pair, summed_pair, buf, sem)

    def per_band(values):
        return sum(values[r * bands : (r + 1) * bands] for r in range(1, 4)) + values[:bands]

    def summed(values):
        return per_band(jnp.sum(values, axis=1, keepdims=True))

    def as_row(column, first):
        shape = (column.shape[0], LANES)
        chosen = iota(shape, 1) == iota(shape, 0) + first
        return jnp.sum(jnp.where(chosen, column, 0.0), axis=0, keepdims=True)

    def as_column(row, first):
        shape = (bands, LANES)
        chosen = iota(shape, 1) == iota(shape, 0) + first
        return jnp.sum(jnp.where(chosen, row, 0.0), axis=1, keepdims=True)

    def lanes_per_band(row, first):
        row = row + pltpu.roll(row, LANES // 2, 1)
        row = row + pltpu.roll(row, LANES // 4, 1)
        lane = iota(row.shape, 1)
        return jnp.where((lane >= first) & (lane < first + bands), row, 0.0)

    def down_rows(column):
        return jnp.concatenate([column] * 4, 0)

    diag = jnp.concatenate([diag_ref[...]] * 2, 1)
    stren = str_ref[...]

    forth(vec, sendb, recvb, 0)
    project(vec, cpart, cpair, csum, crs, cm)
    d = vec[...]
    scal_row = as_row(summed(diag * d * d), 0) + as_row(summed(d * d), 2 * bands)
    owners_tell(crs, cfull, cm)
    field = fields(recvb, 0)
    field_ref[...] = field
    pot = jnp.concatenate([pots_ref[...]] * 2, 0)
    weighted = field * pot
    energy = jnp.sum(weighted * field, axis=0, keepdims=True)
    sendc[...] = triple((t3h_ref[...], t3l_ref[...]), halves(weighted)).reshape(sendc.shape)
    exchange(sendc, recvc, es.at[1], er.at[1])
    scal[0] = scal_row + lanes_per_band(energy, 0)
    add_up(scal, spair, scals, sm)

    told(cfull, cm)
    coupled = cfull[...].reshape(2 * bands, every)
    weights = halves(coupled * stren)
    for r in range(4):
        at = slice(r * every, (r + 1) * every)
        rows = slice(r * bands, (r + 1) * bands)
        mixed = triple(weights, (ph_ref[at, :], pl_ref[at, :]))
        img[rows, :half] = mixed[:bands, :half] - mixed[bands:, half:]
        img[rows, half:] = mixed[:bands, half:] + mixed[bands:, :half]
    pair = jnp.sum(stren * coupled * coupled, axis=1, keepdims=True)
    own_pair = points * (pair[:bands] + pair[bands:])
    totals = added_up(scals, sm)
    norm_now = as_column(totals, 2 * bands)
    curvature = as_column(totals, 0) + own_pair
    alpha = norm_now / curvature

    arrived(recvc, n - 1, er.at[1])
    back = swap_blocks(recvc[...]).reshape(n * TILE, LANES).T
    smooth = triple(halves(back), (t2h_ref[...], t2l_ref[...]))
    d = vec[...]
    image = diag * d + smooth + img[...]
    res[...] = d - down_rows(alpha) * image

    forth(res, sende, recve, 2)
    project(res, cpart2, cpair2, csum2, crs2, cm2)
    d, r2 = vec[...], res[...]
    stiff = diag * r2
    row2 = as_row(summed(stiff * r2), 0) + as_row(summed(stiff * d), bands)
    row2 = row2 + as_row(summed(r2 * r2), 2 * bands)
    scal2[0] = row2
    owns2, tile2 = owner_of(cpart2.shape[0])

    @pl.when(owns2)
    def _():
        arrived(crs2, chips - 1, cm2.at[3])
        t = tile2
        mine = jnp.sum(crs2[...], axis=0)
        old = cfull[pl.ds(t, 1)].reshape(TILE, every)
        first = lax.rem(t * TILE, bands)
        with_mine = points * jnp.sum(stren * mine * mine, axis=1, keepdims=True)
        with_old = points * jnp.sum(stren * mine * old, axis=1, keepdims=True)
        scal2[0] = scal2[0] + as_row(with_mine, first) + as_row(with_old, first + bands)

    field2 = fields(recve, 2)
    weighted2 = field2 * jnp.concatenate([pots_ref[...]] * 2, 0)
    own2 = jnp.sum(weighted2 * field2, axis=0, keepdims=True)
    cross2 = jnp.sum(weighted2 * field_ref[...], axis=0, keepdims=True)
    scal2[0] = scal2[0] + lanes_per_band(own2, 0) + lanes_per_band(cross2, bands)
    add_up(scal2, spair2, scals2, sm2)
    totals2 = added_up(scals2, sm2)
    norm_next = as_column(totals2, 2 * bands)
    beta = norm_next / norm_now
    curvature2 = (
        as_column(totals2, 0) + 2.0 * beta * as_column(totals2, bands) + beta * beta * curvature
    )
    alpha2 = norm_next / curvature2
    of_first = alpha + alpha2 * beta
    for r in range(4):
        rows = slice(r * bands, (r + 1) * bands)
        total = of_first * vec[rows, :] + alpha2 * res[rows, :]
        for part in range(2):
            sol_raw[:, part, r, :] = total[:, part * half : (part + 1) * half]

    for copy in to_right + to_left + [far_right, far_left, far_f, far_b]:
        copy.wait_send()
    across.wait_send()
    swap.wait_send()
    sent_to_owners(mpart, msum, mm)
    owners_done(mrs, mfull, mm)
    sent_to_owners(cpart, csum, cm)
    owners_done(crs, cfull, cm)
    sent_to_owners(cpart2, csum2, cm2)
    left_here(sendb, n - 1, es.at[0])
    left_here(sendc, n - 1, es.at[1])
    left_here(sende, n - 1, es.at[2])
    adding_done(scal, scals, sm)
    adding_done(scal2, scals2, sm2)


def centred(index, length):
    shifted = (index + length // 2) % length - length // 2
    return shifted.astype(jnp.float32) / length


def split_table(table):
    table = table.astype(np.float32)
    high = table.astype(ml_dtypes.bfloat16)
    low = (table - high.astype(np.float32)).astype(ml_dtypes.bfloat16)
    return high, low


def tables(length, peers):
    index = np.arange(length)
    angle = (index[:, None] * index[None, :] % length) * (2.0 * math.pi / length)
    cosine, sine = np.cos(angle) / math.sqrt(length), np.sin(angle) / math.sqrt(length)
    out = np.block([[cosine, -sine], [sine, cosine]])
    order = np.arange(2 * length).reshape(2, peers, length // peers).transpose(1, 0, 2).reshape(-1)
    return split_table(out[order])


def body(n, nx, waves, forward, backward, projectors, potential, strengths, shifts):
    bands, parts, rows, width = waves.shape
    length = rows * n
    points = float(length * width)
    every = nx * bands
    count = projectors.shape[0]
    shape = (rows * bands, parts * width)
    f32 = functools.partial(pltpu.VMEM, dtype=jnp.float32)
    full, line, tiles = (n, TILE, LANES), (n // 2, TILE, LANES), 2 * bands // TILE
    vmem = pl.BlockSpec(memory_space=pltpu.VMEM)
    dma = pltpu.SemaphoreType.DMA
    der, sol = pl.pallas_call(
        functools.partial(kernel, n, nx, points),
        out_shape=[jax.ShapeDtypeStruct(waves.shape, jnp.float32)] * 2,
        in_specs=[vmem] * 9,
        out_specs=[vmem] * 2,
        scratch_shapes=[
            f32(shape), f32(shape), f32(shape),
            f32((rows * bands, width)), f32((length, LANES)),
            *[pltpu.VMEM((rows * count, parts * width), jnp.bfloat16)] * 2,
            *[pltpu.VMEM((2 * length, 2 * length), jnp.bfloat16)] * 4,
            f32((nx, *shape)), f32((2, every, every)),
            f32((nx, 2, *shape)),
            f32((2 * tiles, TILE, LANES)), *[f32((tiles, TILE, LANES))] * 2, f32(line),
            f32((2 * tiles, TILE, LANES)),
            f32((nx, 2 * tiles, TILE, LANES)), f32((2, every, every)), f32((2, 2 * bands, every)),
            f32(shape), f32(shape), f32(shape),
            f32(full), f32(full), f32(full), f32(full), f32(full), f32(full),
            f32((tiles, TILE, LANES)), *[f32((tiles // 2, TILE, LANES))] * 2, f32(line),
            f32((tiles, TILE, LANES)),
            f32((tiles, TILE, LANES)), *[f32((tiles // 2, TILE, LANES))] * 2, f32(line),
            *[f32((2, 1, LANES)), f32((1, LANES)), f32((n // 2, 1, LANES))] * 2,
            f32((n * TILE, LANES)),
            pltpu.SemaphoreType.REGULAR((n.bit_length(),)),
            dma((12,)), dma((12,)), dma, dma, dma, dma, dma((8,)), dma((8,)), dma((8,)), dma((4,)), dma((4,)),
            dma((3,)), dma((3,)),
        ],
        compiler_params=pltpu.CompilerParams(
            collective_id=0, has_side_effects=True, vmem_limit_bytes=60 * 1024 * 1024
        ),
    )(
        waves, forward, backward, projectors, jnp.tile(shifts, rows).reshape(-1, 1), potential,
        strengths.reshape(1, count), *[jnp.asarray(t) for t in tables(length, n)],
    )

    return sol, der


def solution(mesh):
    bands = P("band", "kgrp", "pw", None)
    return jax.shard_map(
        functools.partial(body, mesh.shape["pw"], mesh.shape["band"]),
        mesh=mesh,
        in_specs=(bands, bands, bands, P("kgrp", None, "pw", None), P("pw", None), P(), P("band")),
        out_specs=(bands, bands),
        check_vma=False,
    )
```

```python
import functools
import math

import jax
import jax.numpy as jnp
import ml_dtypes
import numpy as np
from jax import lax
from jax.experimental import pallas as pl
from jax.experimental.pallas import tpu as pltpu
from jax.sharding import PartitionSpec as P

MESH = pl.DeviceIdType.MESH
HIGHEST = lax.Precision.HIGHEST
string_step = 0.05
kinetic_scale = 4.0
LANES = 128
TILE = 8

NN = (((1,), (0,)), ((), ()))
NT = (((1,), (1,)), ((), ()))


def exact(a, b, dims=NN):
    return lax.dot_general(a, b, dims, precision=HIGHEST, preferred_element_type=jnp.float32)


def single(a, b, dims):
    return lax.dot_general(a, b, dims, preferred_element_type=jnp.float32)


def halves(a):
    high = a.astype(jnp.bfloat16)
    low = (a - high.astype(jnp.float32)).astype(jnp.bfloat16)
    return high, low


def triple(a, b, dims=NN):
    (ah, al), (bh, bl) = a, b
    return single(ah, bh, dims) + (single(ah, bl, dims) + single(al, bh, dims))


def iota(shape, dim):
    return lax.broadcasted_iota(jnp.int32, shape, dim)


def swap_blocks(tiles):
    u = iota(tiles.shape, 1) % 4
    w = iota(tiles.shape, 2) // (LANES // 4)
    turned = pltpu.roll(tiles, LANES // 2, 2)
    below, above = pltpu.roll(turned, TILE - 2, 1), pltpu.roll(turned, 2, 1)
    same, upper = (u // 2) == (w // 2), (u // 2) < (w // 2)
    tiles = jnp.where(same, tiles, jnp.where(upper, below, above))
    below = pltpu.roll(pltpu.roll(tiles, LANES // 4, 2), TILE - 1, 1)
    above = pltpu.roll(pltpu.roll(tiles, LANES - LANES // 4, 2), 1, 1)
    same, upper = (u % 2) == (w % 2), (u % 2) < (w % 2)
    return jnp.where(same, tiles, jnp.where(upper, below, above))


def kernel(
    n, nx, points,
    w_raw, f_raw, b_raw, p_ref, shift_ref, pot_ref, str_ref,
    t2h_ref, t2l_ref,
    der_raw, sol_raw,
    w_ref, f_ref, b_ref,
    diag_ref, pots_ref, ph_ref, pl_ref, t1h_ref, t1l_ref, t3h_ref, t3l_ref, wide, qt, near, mpart, mpair, msum, mrs, mfull, mall, nmat, zmat,
    vec, res, img,
    sendb, recvb, sendc, recvc, sende, recve,
    cpart, cpair, csum, crs, cfull, cpart2, cpair2, csum2, crs2,
    scal, spair, scals, scal2, spair2, scals2, field_ref,
    known, xs, xr, zs, zr_sem, ms, mr, mm, cm, cm2, sm, sm2, es, er,
):
    me = lax.axis_index("pw")
    mx = lax.axis_index("band")
    bands = w_ref.shape[0] // 4
    half = w_ref.shape[1] // 2
    every = nx * bands
    right, left = lax.rem(mx + 1, nx), lax.rem(mx + nx - 1, nx)

    def other(i):
        part = (i + 1) // 2
        return lax.rem(me + n // 2 + part * (2 * lax.rem(i, 2) - 1) + n, n)


    def flatten(raw, flat_ref):
        for r in range(4):
            for part in range(2):
                lanes = slice(part * half, (part + 1) * half)
                flat_ref[r * bands : (r + 1) * bands, lanes] = raw[:, part, r, :]

    barrier = pltpu.get_barrier_semaphore()

    partner = me + 1 - 2 * lax.rem(me, 2)

    def at_distance(d):
        return lax.rem(me + d + n, n)

    def greet(d, axis="pw", base=None):
        target = at_distance(d) if base is None else base
        pl.semaphore_signal(barrier, inc=1, device_id={axis: target}, device_id_type=MESH)

    greet(0, "pw", partner)
    greet(2)
    greet(-2)
    for step in range(1, nx):
        greet(0, "band", lax.rem(mx + step, nx))
    flatten(w_raw, w_ref)
    flatten(f_raw, f_ref)
    flatten(b_raw, b_ref)
    pl.semaphore_wait(barrier, 3 + nx - 1)

    rounds = (n // 4).bit_length() - 1

    def say(k):
        d = 2 << k
        for target in (at_distance(d), at_distance(-d)):
            pl.semaphore_signal(known.at[k], inc=1, device_id={"pw": target}, device_id_type=MESH)

    def hear(k):
        pl.semaphore_wait(known.at[k], 2)

    def learn(k):
        say(k)
        hear(k)

    def say_to_partner():
        pl.semaphore_signal(known.at[rounds], inc=1, device_id={"pw": partner}, device_id_type=MESH)

    def hear_partner():
        pl.semaphore_wait(known.at[rounds], 1)

    def remote(src, dst, send, recv, axis, target):
        return pltpu.make_async_remote_copy(
            src_ref=src, dst_ref=dst, send_sem=send, recv_sem=recv,
            device_id={axis: target}, device_id_type=MESH,
        )

    group = max(k for k in (1, 3, 7, 9) if (n - 1) % k == 0)

    def to_others(start):
        def some(i, carry):
            for k in range(group):
                start(other(i * group + k))
            return carry

        lax.fori_loop(0, (n - 1) // group, some, 0)

    def exchange(src, dst, send, recv):
        dst[pl.ds(me, 1)] = src[pl.ds(me, 1)]
        to_others(lambda t: remote(src.at[t], dst.at[me], send, recv, "pw", t).start())

    core, place, chips = lax.rem(me, 2), me // 2, n // 2

    def line_other(i):
        part = (i + 1) // 2
        chip = lax.rem(place + chips // 2 + part * (2 * lax.rem(i, 2) - 1) + chips, chips)
        return 2 * chip + core

    def tell_line(src, dst, send, recv):
        def one(i, carry):
            remote(src, dst, send, recv, "pw", line_other(i)).start()
            return carry

        lax.fori_loop(0, chips - 1, one, 0)

    def arrived(dst, count, recv):
        some = dst.at[pl.ds(0, count)]
        remote(some, some, recv, recv, "pw", partner).wait_recv()

    def left_here(src, count, send):
        some = src.at[pl.ds(0, count)]
        remote(some, some, send, send, "pw", partner).wait_send()

    def owner_of(tiles):
        stride = chips // (tiles // 2)
        return lax.rem(place, stride) == 0, core * (tiles // 2) + place // stride

    def to_owners(part, pair, summed_pair, dst, sem):
        tiles = part.shape[0] // 2
        stride = chips // tiles
        theirs = pl.ds((1 - core) * tiles, tiles)
        copy = remote(part.at[theirs], pair, sem.at[0], sem.at[1], "pw", partner)
        copy.start()
        copy.wait_recv()
        summed_pair[...] = part[pl.ds(core * tiles, tiles)] + pair[...]

        def one(i, carry):
            t = lax.rem(i + place // stride, tiles)
            owner = 2 * t * stride + core

            @pl.when(owner != me)
            def _():
                remote(
                    summed_pair.at[t], dst.at[place], sem.at[2], sem.at[3], "pw", owner
                ).start()

            @pl.when(owner == me)
            def _():
                dst[pl.ds(place, 1)] = summed_pair[pl.ds(t, 1)]

            return carry

        lax.fori_loop(0, tiles, one, 0)

    def sent_to_owners(part, summed_pair, sem):
        tiles = summed_pair.shape[0]
        owns, _ = owner_of(2 * tiles)
        left_here(part, tiles, sem.at[0])

        @pl.when(owns)
        def _():
            left_here(summed_pair, tiles - 1, sem.at[2])

        @pl.when(jnp.logical_not(owns))
        def _():
            left_here(summed_pair, tiles, sem.at[2])

    def owners_tell(buf, full, sem):
        owns, t = owner_of(full.shape[0])

        @pl.when(owns)
        def _():
            arrived(buf, chips - 1, sem.at[3])
            full[pl.ds(t, 1)] = jnp.sum(buf[...], axis=0, keepdims=True)
            tell_line(full.at[t], full.at[t], sem.at[4], sem.at[5])

    def told(full, sem):
        tiles = full.shape[0] // 2
        owns, _ = owner_of(2 * tiles)

        @pl.when(owns)
        def _():
            arrived(full, tiles - 1, sem.at[5])

        @pl.when(jnp.logical_not(owns))
        def _():
            arrived(full, tiles, sem.at[5])

    def told_chip(full, sem):
        tiles = full.shape[0] // 2
        mine = full.at[pl.ds(core * tiles, tiles)]
        remote(mine, mine, sem.at[6], sem.at[7], "pw", partner).start()
        arrived(full, tiles, sem.at[7])

    def owners_done(buf, full, sem):
        owns, _ = owner_of(full.shape[0])

        @pl.when(owns)
        def _():
            left_here(buf, chips - 1, sem.at[4])

    def add_up(mine, pair, rows, sem):
        remote(mine.at[0], pair, sem.at[0], sem.at[1], "pw", partner).start()
        remote(mine.at[0], pair, sem.at[0], sem.at[1], "pw", partner).wait_recv()
        mine[1] = mine[0] + pair[...]
        tell_line(mine.at[1], rows.at[place], sem.at[2], sem.at[3])
        rows[pl.ds(place, 1)] = mine[1][None]

    def added_up(rows, sem):
        arrived(rows, chips - 1, sem.at[3])
        return jnp.sum(rows[...], axis=0)

    def adding_done(mine, rows, sem):
        remote(mine.at[0], mine.at[0], sem.at[0], sem.at[0], "pw", partner).wait_send()
        left_here(rows, chips - 1, sem.at[2])

    part_rows = w_ref.shape[0] // 2
    lower, upper = pl.ds(0, part_rows), pl.ds(part_rows, part_rows)

    def over_band(src, dst, at, target):
        return remote(src, dst, xs.at[at], xr.at[at], "band", target)

    to_right = [
        over_band(w_ref.at[lower], wide.at[3, lower], 0, right),
        over_band(w_ref.at[upper], wide.at[3, upper], 1, right),
        over_band(f_ref, near.at[3, 0], 6, right),
        over_band(b_ref, near.at[3, 1], 8, right),
    ]
    to_left = [
        over_band(w_ref.at[upper], wide.at[1, upper], 2, left),
        over_band(w_ref.at[lower], wide.at[1, lower], 3, left),
        over_band(b_ref, near.at[1, 1], 9, left),
        over_band(f_ref, near.at[1, 0], 7, left),
    ]
    for a, b in zip(to_right, to_left):
        a.start()
        b.start()
    say(0)
    wide[0] = w_ref[...]
    near[0, 0] = f_ref[...]
    near[0, 1] = b_ref[...]
    hear(0)
    say(1)
    own = []
    for r in range(4):
        both = []
        for src in (f_ref, b_ref):
            rows = src[r * bands : (r + 1) * bands, :]
            both += [rows, jnp.concatenate([rows[:, half:], -rows[:, :half]], 1)]
        own.append(halves(jnp.concatenate(both, 0)))

    def margin_of(slot):
        total = None
        for r in range(4):
            term = triple(own[r], halves(wide[slot, r * bands : (r + 1) * bands, :]), NT)
            total = term if total is None else total + term
        nmat[0, :, slot * bands : (slot + 1) * bands] = total

    hear(1)
    say(2)
    to_right[0].wait_recv()
    far_right = over_band(wide.at[3, lower], wide.at[2, lower], 4, right)
    far_right.start()
    to_left[0].wait_recv()
    far_left = over_band(wide.at[1, upper], wide.at[2, upper], 5, left)
    far_left.start()
    hear(2)
    for k in range(3, rounds - 1):
        learn(k)
    if rounds > 3:
        say(rounds - 1)
    margin_of(0)
    to_right[1].wait_recv()
    margin_of(3)
    to_left[1].wait_recv()
    margin_of(1)
    far_right.wait_recv()
    far_left.wait_recv()
    margin_of(2)
    turned = pltpu.roll(nmat[0], mx * bands, 1)
    mpart[...] = turned.reshape(mpart.shape)
    if rounds > 3:
        hear(rounds - 1)
    say_to_partner()

    to_owners(mpart, mpair, msum, mrs, mm)
    for r in range(4):
        for part in range(2):
            rows = slice(r * every, (r + 1) * every)
            lanes = slice(part * half, (part + 1) * half)
            ph_ref[rows, lanes], pl_ref[rows, lanes] = halves(p_ref[:, part, r, :])
    u = me * 4 + iota((4 * bands, half), 0) // bands
    w = iota((4 * bands, half), 1)
    u, w = centred(u, 4 * n), centred(w, half)
    diag_ref[...] = kinetic_scale * (u * u + w * w) + shift_ref[...]
    columns = jnp.concatenate([pot_ref[...]] * 2, 0).T
    at = iota((4 * n, LANES), 1) // bands
    spread = jnp.zeros((4 * n, LANES), jnp.float32)
    for k in range(4):
        spread = jnp.where(at == k, columns[:, k : k + 1], spread)
    pots_ref[...] = spread
    shape = t2h_ref.shape
    row_part, lane_part = iota(shape, 0) % TILE // (TILE // 2), iota(shape, 1) // half
    flip = jnp.where(row_part == lane_part, 1.0, -1.0)
    inverse_table = (t2h_ref[...].astype(jnp.float32) + t2l_ref[...].astype(jnp.float32)) * flip
    t3h_ref[...], t3l_ref[...] = halves(inverse_table)
    t1h_ref[...], t1l_ref[...] = halves(inverse_table.T)
    owners_tell(mrs, mfull, mm)
    to_right[2].wait_recv()
    far_f = over_band(near.at[3, 0], near.at[2, 0], 10, right)
    far_f.start()
    to_left[2].wait_recv()
    far_b = over_band(near.at[1, 1], near.at[2, 1], 11, left)
    far_b.start()
    told(mfull, mm)
    mine_half = pl.ds(core * (mfull.shape[0] // 2), mfull.shape[0] // 2)
    mall[pl.ds(mx, 1)] = mfull[mine_half][None]
    for step in range(1, nx):
        t = lax.rem(mx + step, nx)
        remote(mfull.at[mine_half], mall.at[mx], ms, mr, "band", t).start()
    some = mall.at[pl.ds(0, nx - 1)]
    across = remote(some, some, ms, mr, "band", right)
    across.wait_recv()

    def margin_full(part):
        tiles_each = bands // TILE
        at = slice(part * tiles_each, (part + 1) * tiles_each)
        rows = [mall[x, at].reshape(bands, every) for x in range(nx)]
        return jnp.concatenate(rows, 0) / points

    real, imag = margin_full(0), margin_full(1)
    nmat[0] = exact(real, real, NT) + exact(imag, imag, NT)
    nmat[1] = exact(imag, real, NT) - exact(real, imag, NT)
    qt[0] = real.T
    qt[1] = imag.T

    def times(a, b):
        return a[0] * b[0] - a[1] * b[1], a[0] * b[1] + a[1] * b[0]

    def minus(a, b):
        return a[0] - b[0], a[1] - b[1]

    def conj(a):
        return a[0], -a[1]

    def solver(first, last, across):
        scale = 1.0 / (first * last - across[0] * across[0] - across[1] * across[1])
        first, last = first * scale, last * scale
        across = (across[0] * scale, across[1] * scale)

        def solve(x, y):
            new_x = minus((last * x[0], last * x[1]), times(across, y))
            return new_x, minus((first * y[0], first * y[1]), times(conj(across), x))

        return solve

    def eliminate(step, carry):
        c = 4 * step
        lane = iota((every, every), 1)
        at_0 = jnp.full((every, every), 0, jnp.int32) + c
        line = iota((1, every), 1)
        lows, highs = (line == c) | (line == c + 1), (line == c + 2) | (line == c + 3)
        on = (lane >= c) & (lane < c + 4)

        def without(row, where):
            return jnp.where(where, 0.0, row[0]), jnp.where(where, 0.0, row[1])

        def unit(row, where, k):
            return jnp.where(where, jnp.where(line == c + k, 1.0, 0.0), row[0]), jnp.where(where, 0.0, row[1])

        real, imag = nmat[0], nmat[1]
        rows = [
            (nmat[0, pl.ds(c + k, 1), :], nmat[1, pl.ds(c + k, 1), :])
            for k in range(4)
        ]

        def one(row, k):
            return jnp.sum(jnp.where(line == c + k, row, 0.0), axis=1, keepdims=True)

        def element(j, k):
            return one(rows[j][0], k), one(rows[j][1], k)

        diag4 = [one(rows[k][0], k) for k in range(4)]
        off = {(j, k): element(j, k) for j in range(4) for k in range(j + 1, 4)}
        solve = solver(diag4[0], diag4[1], off[0, 1])
        head = {k: solve(off[0, k], off[1, k]) for k in (2, 3)}

        def rest(j, k, value):
            value = minus(value, times(conj(off[0, j]), head[k][0]))
            return minus(value, times(conj(off[1, j]), head[k][1]))

        zero = jnp.zeros_like(diag4[2])
        last_solve = solver(
            rest(2, 2, (diag4[2], zero))[0], rest(3, 3, (diag4[3], zero))[0], rest(2, 3, off[2, 3])
        )
        new = list(solve(unit(rows[0], lows, 0), unit(rows[1], lows, 1)))
        tail = []
        for k in (2, 3):
            row = minus(without(rows[k], lows), times(conj(off[0, k]), new[0]))
            row = minus(row, times(conj(off[1, k]), new[1]))
            tail.append(unit(row, highs, k))
        tail = last_solve(*tail)
        for k in range(2):
            row = minus(without(new[k], highs), times(head[2][k], tail[0]))
            new[k] = minus(row, times(head[3][k], tail[1]))
        new += tail
        total = jnp.where(on, 0.0, real), jnp.where(on, 0.0, imag)
        for k in range(4):
            column = (
                jnp.take_along_axis(real, at_0 + k, axis=1),
                jnp.take_along_axis(imag, at_0 + k, axis=1),
            )
            total = minus(total, times(column, new[k]))
        nmat[0], nmat[1] = total
        for k in range(4):
            nmat[0, pl.ds(c + k, 1), :] = new[k][0]
            nmat[1, pl.ds(c + k, 1), :] = new[k][1]
        return carry

    lax.fori_loop(0, every // 4, eliminate, 0)

    mine = pl.ds(pl.multiple_of(mx * bands, TILE), bands)
    qr, qi = qt[0, mine, :], qt[1, mine, :]
    nr, ni = nmat[0], nmat[1]
    zr = exact(qr, nr) + exact(qi, ni)
    zi = exact(qr, ni) - exact(qi, nr)
    both = pltpu.roll(jnp.concatenate([zr, zi], 0), lax.rem((nx - mx) * bands, every), 1)
    zmat[pl.ds(core, 1)] = jnp.where(core == 0, both, -both)[None]
    swap = remote(zmat.at[core], zmat.at[core], zs, zr_sem, "pw", partner)
    swap.start()

    to_right[3].wait_recv()
    to_left[3].wait_recv()
    far_f.wait_recv()
    far_b.wait_recv()
    hear_partner()
    swap.wait_recv()
    coeff = jnp.concatenate([zmat[0], zmat[1]], 1)
    for r in range(4):
        rows = slice(r * bands, (r + 1) * bands)
        blocks = [near[d, which, rows, :] for which in range(2) for d in range(nx)]
        mixed = exact(coeff, jnp.concatenate(blocks, 0))
        dr = (mixed[:bands, :half] - mixed[bands:, half:]) / (2.0 * string_step)
        di = (mixed[:bands, half:] + mixed[bands:, :half]) / (2.0 * string_step)
        der_raw[:, 0, r, :] = dr
        der_raw[:, 1, r, :] = di
        vec[rows, :half] = -dr
        vec[rows, half:] = -di

    def forth(src, send, recv, sem):
        parts = halves(src[...])
        out = triple((t2h_ref[...], t2l_ref[...]), parts, NT)
        send[...] = swap_blocks(out.reshape(n, TILE, LANES))
        exchange(send, recv, es.at[sem], er.at[sem])

    def fields(recv, sem):
        arrived(recv, n - 1, er.at[sem])
        parts = halves(recv[...].reshape(n * TILE, LANES))
        return triple((t1h_ref[...], t1l_ref[...]), parts)

    def project(src, part, pair, summed_pair, buf, sem):
        total = None
        for r in range(4):
            rows = src[r * bands : (r + 1) * bands, :]
            both = jnp.concatenate([rows, jnp.concatenate([rows[:, half:], -rows[:, :half]], 1)], 0)
            at = slice(r * every, (r + 1) * every)
            term = triple(halves(both), (ph_ref[at, :], pl_ref[at, :]), NT)
            total = term if total is None else total + term
        part[...] = (total / points).reshape(part.shape)
        to_owners(part, pair, summed_pair, buf, sem)

    def per_band(values):
        return sum(values[r * bands : (r + 1) * bands] for r in range(1, 4)) + values[:bands]

    def summed(values):
        return per_band(jnp.sum(values, axis=1, keepdims=True))

    def as_row(column, first):
        shape = (column.shape[0], LANES)
        chosen = iota(shape, 1) == iota(shape, 0) + first
        return jnp.sum(jnp.where(chosen, column, 0.0), axis=0, keepdims=True)

    def as_column(row, first):
        shape = (bands, LANES)
        chosen = iota(shape, 1) == iota(shape, 0) + first
        return jnp.sum(jnp.where(chosen, row, 0.0), axis=1, keepdims=True)

    def lanes_per_band(row, first):
        row = row + pltpu.roll(row, LANES // 2, 1)
        row = row + pltpu.roll(row, LANES // 4, 1)
        lane = iota(row.shape, 1)
        return jnp.where((lane >= first) & (lane < first + bands), row, 0.0)

    def down_rows(column):
        return jnp.concatenate([column] * 4, 0)

    diag = jnp.concatenate([diag_ref[...]] * 2, 1)
    stren = str_ref[...]

    forth(vec, sendb, recvb, 0)
    project(vec, cpart, cpair, csum, crs, cm)
    d = vec[...]
    scal_row = as_row(summed(diag * d * d), 0) + as_row(summed(d * d), 2 * bands)
    owners_tell(crs, cfull, cm)
    field = fields(recvb, 0)
    field_ref[...] = field
    pot = jnp.concatenate([pots_ref[...]] * 2, 0)
    weighted = field * pot
    energy = jnp.sum(weighted * field, axis=0, keepdims=True)
    sendc[...] = triple((t3h_ref[...], t3l_ref[...]), halves(weighted)).reshape(sendc.shape)
    exchange(sendc, recvc, es.at[1], er.at[1])
    scal[0] = scal_row + lanes_per_band(energy, 0)
    add_up(scal, spair, scals, sm)

    told(cfull, cm)
    told_chip(cfull, cm)
    coupled = cfull[...].reshape(2 * bands, every)
    weights = halves(coupled * stren)
    for r in range(4):
        at = slice(r * every, (r + 1) * every)
        rows = slice(r * bands, (r + 1) * bands)
        mixed = triple(weights, (ph_ref[at, :], pl_ref[at, :]))
        img[rows, :half] = mixed[:bands, :half] - mixed[bands:, half:]
        img[rows, half:] = mixed[:bands, half:] + mixed[bands:, :half]
    pair = jnp.sum(stren * coupled * coupled, axis=1, keepdims=True)
    own_pair = points * (pair[:bands] + pair[bands:])
    totals = added_up(scals, sm)
    norm_now = as_column(totals, 2 * bands)
    curvature = as_column(totals, 0) + own_pair
    alpha = norm_now / curvature

    arrived(recvc, n - 1, er.at[1])
    back = swap_blocks(recvc[...]).reshape(n * TILE, LANES).T
    smooth = triple(halves(back), (t2h_ref[...], t2l_ref[...]))
    d = vec[...]
    image = diag * d + smooth + img[...]
    res[...] = d - down_rows(alpha) * image

    forth(res, sende, recve, 2)
    project(res, cpart2, cpair2, csum2, crs2, cm2)
    d, r2 = vec[...], res[...]
    stiff = diag * r2
    row2 = as_row(summed(stiff * r2), 0) + as_row(summed(stiff * d), bands)
    row2 = row2 + as_row(summed(r2 * r2), 2 * bands)
    scal2[0] = row2
    owns2, tile2 = owner_of(cpart2.shape[0])

    @pl.when(owns2)
    def _():
        arrived(crs2, chips - 1, cm2.at[3])
        t = tile2
        mine = jnp.sum(crs2[...], axis=0)
        old = cfull[pl.ds(t, 1)].reshape(TILE, every)
        first = lax.rem(t * TILE, bands)
        with_mine = points * jnp.sum(stren * mine * mine, axis=1, keepdims=True)
        with_old = points * jnp.sum(stren * mine * old, axis=1, keepdims=True)
        scal2[0] = scal2[0] + as_row(with_mine, first) + as_row(with_old, first + bands)

    field2 = fields(recve, 2)
    weighted2 = field2 * jnp.concatenate([pots_ref[...]] * 2, 0)
    own2 = jnp.sum(weighted2 * field2, axis=0, keepdims=True)
    cross2 = jnp.sum(weighted2 * field_ref[...], axis=0, keepdims=True)
    scal2[0] = scal2[0] + lanes_per_band(own2, 0) + lanes_per_band(cross2, bands)
    add_up(scal2, spair2, scals2, sm2)
    totals2 = added_up(scals2, sm2)
    norm_next = as_column(totals2, 2 * bands)
    beta = norm_next / norm_now
    curvature2 = (
        as_column(totals2, 0) + 2.0 * beta * as_column(totals2, bands) + beta * beta * curvature
    )
    alpha2 = norm_next / curvature2
    of_first = alpha + alpha2 * beta
    for r in range(4):
        rows = slice(r * bands, (r + 1) * bands)
        total = of_first * vec[rows, :] + alpha2 * res[rows, :]
        for part in range(2):
            sol_raw[:, part, r, :] = total[:, part * half : (part + 1) * half]

    for copy in to_right + to_left + [far_right, far_left, far_f, far_b]:
        copy.wait_send()
    across.wait_send()
    swap.wait_send()
    sent_to_owners(mpart, msum, mm)
    owners_done(mrs, mfull, mm)
    sent_to_owners(cpart, csum, cm)
    owners_done(crs, cfull, cm)
    left_here(cfull, cfull.shape[0] // 2, cm.at[6])
    sent_to_owners(cpart2, csum2, cm2)
    left_here(sendb, n - 1, es.at[0])
    left_here(sendc, n - 1, es.at[1])
    left_here(sende, n - 1, es.at[2])
    adding_done(scal, scals, sm)
    adding_done(scal2, scals2, sm2)


def centred(index, length):
    shifted = (index + length // 2) % length - length // 2
    return shifted.astype(jnp.float32) / length


def split_table(table):
    table = table.astype(np.float32)
    high = table.astype(ml_dtypes.bfloat16)
    low = (table - high.astype(np.float32)).astype(ml_dtypes.bfloat16)
    return high, low


def tables(length, peers):
    index = np.arange(length)
    angle = (index[:, None] * index[None, :] % length) * (2.0 * math.pi / length)
    cosine, sine = np.cos(angle) / math.sqrt(length), np.sin(angle) / math.sqrt(length)
    out = np.block([[cosine, -sine], [sine, cosine]])
    order = np.arange(2 * length).reshape(2, peers, length // peers).transpose(1, 0, 2).reshape(-1)
    return split_table(out[order])


def body(n, nx, waves, forward, backward, projectors, potential, strengths, shifts):
    bands, parts, rows, width = waves.shape
    length = rows * n
    points = float(length * width)
    every = nx * bands
    count = projectors.shape[0]
    shape = (rows * bands, parts * width)
    f32 = functools.partial(pltpu.VMEM, dtype=jnp.float32)
    full, line, tiles = (n, TILE, LANES), (n // 2, TILE, LANES), 2 * bands // TILE
    vmem = pl.BlockSpec(memory_space=pltpu.VMEM)
    dma = pltpu.SemaphoreType.DMA
    der, sol = pl.pallas_call(
        functools.partial(kernel, n, nx, points),
        out_shape=[jax.ShapeDtypeStruct(waves.shape, jnp.float32)] * 2,
        in_specs=[vmem] * 9,
        out_specs=[vmem] * 2,
        scratch_shapes=[
            f32(shape), f32(shape), f32(shape),
            f32((rows * bands, width)), f32((length, LANES)),
            *[pltpu.VMEM((rows * count, parts * width), jnp.bfloat16)] * 2,
            *[pltpu.VMEM((2 * length, 2 * length), jnp.bfloat16)] * 4,
            f32((nx, *shape)), f32((2, every, every)),
            f32((nx, 2, *shape)),
            f32((2 * tiles, TILE, LANES)), *[f32((tiles, TILE, LANES))] * 2, f32(line),
            f32((2 * tiles, TILE, LANES)),
            f32((nx, tiles, TILE, LANES)), f32((2, every, every)), f32((2, 2 * bands, every)),
            f32(shape), f32(shape), f32(shape),
            f32(full), f32(full), f32(full), f32(full), f32(full), f32(full),
            f32((tiles, TILE, LANES)), *[f32((tiles // 2, TILE, LANES))] * 2, f32(line),
            f32((tiles, TILE, LANES)),
            f32((tiles, TILE, LANES)), *[f32((tiles // 2, TILE, LANES))] * 2, f32(line),
            *[f32((2, 1, LANES)), f32((1, LANES)), f32((n // 2, 1, LANES))] * 2,
            f32((n * TILE, LANES)),
            pltpu.SemaphoreType.REGULAR((n.bit_length(),)),
            dma((12,)), dma((12,)), dma, dma, dma, dma, dma((8,)), dma((8,)), dma((8,)), dma((4,)), dma((4,)),
            dma((3,)), dma((3,)),
        ],
        compiler_params=pltpu.CompilerParams(
            collective_id=0, has_side_effects=True, vmem_limit_bytes=60 * 1024 * 1024
        ),
    )(
        waves, forward, backward, projectors, jnp.tile(shifts, rows).reshape(-1, 1), potential,
        strengths.reshape(1, count), *[jnp.asarray(t) for t in tables(length, n)],
    )

    return sol, der


def solution(mesh):
    bands = P("band", "kgrp", "pw", None)
    return jax.shard_map(
        functools.partial(body, mesh.shape["pw"], mesh.shape["band"]),
        mesh=mesh,
        in_specs=(bands, bands, bands, P("kgrp", None, "pw", None), P("pw", None), P(), P("band")),
        out_specs=(bands, bands),
        check_vma=False,
    )
```

```python
import functools
import math

import jax
import jax.numpy as jnp
import ml_dtypes
import numpy as np
from jax import lax
from jax.experimental import pallas as pl
from jax.experimental.pallas import tpu as pltpu
from jax.sharding import PartitionSpec as P

MESH = pl.DeviceIdType.MESH
HIGHEST = lax.Precision.HIGHEST
string_step = 0.05
kinetic_scale = 4.0
LANES = 128
TILE = 8

NN = (((1,), (0,)), ((), ()))
NT = (((1,), (1,)), ((), ()))


def exact(a, b, dims=NN):
    return lax.dot_general(a, b, dims, precision=HIGHEST, preferred_element_type=jnp.float32)


def single(a, b, dims):
    return lax.dot_general(a, b, dims, preferred_element_type=jnp.float32)


def halves(a):
    high = a.astype(jnp.bfloat16)
    low = (a - high.astype(jnp.float32)).astype(jnp.bfloat16)
    return high, low


def triple(a, b, dims=NN):
    (ah, al), (bh, bl) = a, b
    return single(ah, bh, dims) + (single(ah, bl, dims) + single(al, bh, dims))


def iota(shape, dim):
    return lax.broadcasted_iota(jnp.int32, shape, dim)


def swap_blocks(tiles):
    u = iota(tiles.shape, 1) % 4
    w = iota(tiles.shape, 2) // (LANES // 4)
    turned = pltpu.roll(tiles, LANES // 2, 2)
    below, above = pltpu.roll(turned, TILE - 2, 1), pltpu.roll(turned, 2, 1)
    same, upper = (u // 2) == (w // 2), (u // 2) < (w // 2)
    tiles = jnp.where(same, tiles, jnp.where(upper, below, above))
    below = pltpu.roll(pltpu.roll(tiles, LANES // 4, 2), TILE - 1, 1)
    above = pltpu.roll(pltpu.roll(tiles, LANES - LANES // 4, 2), 1, 1)
    same, upper = (u % 2) == (w % 2), (u % 2) < (w % 2)
    return jnp.where(same, tiles, jnp.where(upper, below, above))


def kernel(
    n, nx, points,
    w_raw, f_raw, b_raw, p_ref, shift_ref, pot_ref, str_ref,
    t2h_ref, t2l_ref,
    der_raw, sol_raw,
    w_ref, f_ref, b_ref,
    diag_ref, pots_ref, ph_ref, pl_ref, t1h_ref, t1l_ref, t3h_ref, t3l_ref, wide, qt, near, mpart, mpair, msum, mrs, mfull, mall, nmat, zmat,
    vec, res, img,
    sendb, recvb, sendc, recvc, sende, recve,
    cpart, cpair, csum, crs, cfull, cpart2, cpair2, csum2, crs2,
    scal, spair, scals, scal2, spair2, scals2, field_ref,
    known, xs, xr, zs, zr_sem, ms, mr, mm, cm, cm2, sm, sm2, es, er,
):
    me = lax.axis_index("pw")
    mx = lax.axis_index("band")
    bands = w_ref.shape[0] // 4
    half = w_ref.shape[1] // 2
    every = nx * bands
    right, left = lax.rem(mx + 1, nx), lax.rem(mx + nx - 1, nx)

    def other(i):
        part = (i + 1) // 2
        return lax.rem(me + n // 2 + part * (2 * lax.rem(i, 2) - 1) + n, n)


    def flatten(raw, flat_ref):
        for r in range(4):
            for part in range(2):
                lanes = slice(part * half, (part + 1) * half)
                flat_ref[r * bands : (r + 1) * bands, lanes] = raw[:, part, r, :]

    barrier = pltpu.get_barrier_semaphore()

    partner = me + 1 - 2 * lax.rem(me, 2)

    def at_distance(d):
        return lax.rem(me + d + n, n)

    def greet(d, axis="pw", base=None):
        target = at_distance(d) if base is None else base
        pl.semaphore_signal(barrier, inc=1, device_id={axis: target}, device_id_type=MESH)

    greet(0, "pw", partner)
    greet(2)
    greet(-2)
    for step in range(1, nx):
        greet(0, "band", lax.rem(mx + step, nx))
    flatten(w_raw, w_ref)
    flatten(f_raw, f_ref)
    flatten(b_raw, b_ref)
    pl.semaphore_wait(barrier, 3 + nx - 1)

    rounds = (n // 4).bit_length() - 1

    def say(k):
        d = 2 << k
        for target in (at_distance(d), at_distance(-d)):
            pl.semaphore_signal(known.at[k], inc=1, device_id={"pw": target}, device_id_type=MESH)

    def hear(k):
        pl.semaphore_wait(known.at[k], 2)

    def learn(k):
        say(k)
        hear(k)

    def say_to_partner():
        pl.semaphore_signal(known.at[rounds], inc=1, device_id={"pw": partner}, device_id_type=MESH)

    def hear_partner():
        pl.semaphore_wait(known.at[rounds], 1)

    def remote(src, dst, send, recv, axis, target):
        return pltpu.make_async_remote_copy(
            src_ref=src, dst_ref=dst, send_sem=send, recv_sem=recv,
            device_id={axis: target}, device_id_type=MESH,
        )

    group = max(k for k in (1, 3, 7, 9) if (n - 1) % k == 0)

    def to_others(start):
        def some(i, carry):
            for k in range(group):
                start(other(i * group + k))
            return carry

        lax.fori_loop(0, (n - 1) // group, some, 0)

    def exchange(src, dst, send, recv):
        dst[pl.ds(me, 1)] = src[pl.ds(me, 1)]
        to_others(lambda t: remote(src.at[t], dst.at[me], send, recv, "pw", t).start())

    core, place, chips = lax.rem(me, 2), me // 2, n // 2

    def line_other(i):
        part = (i + 1) // 2
        chip = lax.rem(place + chips // 2 + part * (2 * lax.rem(i, 2) - 1) + chips, chips)
        return 2 * chip + core

    def tell_line(src, dst, send, recv):
        def one(i, carry):
            remote(src, dst, send, recv, "pw", line_other(i)).start()
            return carry

        lax.fori_loop(0, chips - 1, one, 0)

    def arrived(dst, count, recv):
        some = dst.at[pl.ds(0, count)]
        remote(some, some, recv, recv, "pw", partner).wait_recv()

    def left_here(src, count, send):
        some = src.at[pl.ds(0, count)]
        remote(some, some, send, send, "pw", partner).wait_send()

    def owner_of(tiles):
        stride = chips // (tiles // 2)
        return lax.rem(place, stride) == 0, core * (tiles // 2) + place // stride

    def to_partner(part, pair, sem):
        tiles = part.shape[0] // 2
        theirs = pl.ds((1 - core) * tiles, tiles)
        return remote(part.at[theirs], pair, sem.at[0], sem.at[1], "pw", partner)

    def to_owners(part, pair, summed_pair, dst, sem):
        tiles = part.shape[0] // 2
        stride = chips // tiles
        to_partner(part, pair, sem).wait_recv()
        summed_pair[...] = part[pl.ds(core * tiles, tiles)] + pair[...]

        def one(i, carry):
            t = lax.rem(i + place // stride, tiles)
            owner = 2 * t * stride + core

            @pl.when(owner != me)
            def _():
                remote(
                    summed_pair.at[t], dst.at[place], sem.at[2], sem.at[3], "pw", owner
                ).start()

            @pl.when(owner == me)
            def _():
                dst[pl.ds(place, 1)] = summed_pair[pl.ds(t, 1)]

            return carry

        lax.fori_loop(0, tiles, one, 0)

    def sent_to_owners(part, summed_pair, sem):
        tiles = summed_pair.shape[0]
        owns, _ = owner_of(2 * tiles)
        left_here(part, tiles, sem.at[0])

        @pl.when(owns)
        def _():
            left_here(summed_pair, tiles - 1, sem.at[2])

        @pl.when(jnp.logical_not(owns))
        def _():
            left_here(summed_pair, tiles, sem.at[2])

    def owners_tell(buf, full, sem):
        owns, t = owner_of(full.shape[0])

        @pl.when(owns)
        def _():
            arrived(buf, chips - 1, sem.at[3])
            full[pl.ds(t, 1)] = jnp.sum(buf[...], axis=0, keepdims=True)
            tell_line(full.at[t], full.at[t], sem.at[4], sem.at[5])

    def told(full, sem):
        tiles = full.shape[0] // 2
        owns, _ = owner_of(2 * tiles)

        @pl.when(owns)
        def _():
            arrived(full, tiles - 1, sem.at[5])

        @pl.when(jnp.logical_not(owns))
        def _():
            arrived(full, tiles, sem.at[5])

    def told_chip(full, sem):
        tiles = full.shape[0] // 2
        mine = full.at[pl.ds(core * tiles, tiles)]
        remote(mine, mine, sem.at[6], sem.at[7], "pw", partner).start()
        arrived(full, tiles, sem.at[7])

    def owners_done(buf, full, sem):
        owns, _ = owner_of(full.shape[0])

        @pl.when(owns)
        def _():
            left_here(buf, chips - 1, sem.at[4])

    def add_up(mine, pair, rows, sem):
        remote(mine.at[0], pair, sem.at[0], sem.at[1], "pw", partner).start()
        remote(mine.at[0], pair, sem.at[0], sem.at[1], "pw", partner).wait_recv()
        mine[1] = mine[0] + pair[...]
        tell_line(mine.at[1], rows.at[place], sem.at[2], sem.at[3])
        rows[pl.ds(place, 1)] = mine[1][None]

    def added_up(rows, sem):
        arrived(rows, chips - 1, sem.at[3])
        return jnp.sum(rows[...], axis=0)

    def adding_done(mine, rows, sem):
        remote(mine.at[0], mine.at[0], sem.at[0], sem.at[0], "pw", partner).wait_send()
        left_here(rows, chips - 1, sem.at[2])

    part_rows = w_ref.shape[0] // 2
    lower, upper = pl.ds(0, part_rows), pl.ds(part_rows, part_rows)

    def over_band(src, dst, at, target):
        return remote(src, dst, xs.at[at], xr.at[at], "band", target)

    to_right = [
        over_band(w_ref.at[lower], wide.at[3, lower], 0, right),
        over_band(w_ref.at[upper], wide.at[3, upper], 1, right),
        over_band(f_ref, near.at[3, 0], 6, right),
        over_band(b_ref, near.at[3, 1], 8, right),
    ]
    to_left = [
        over_band(w_ref.at[upper], wide.at[1, upper], 2, left),
        over_band(w_ref.at[lower], wide.at[1, lower], 3, left),
        over_band(b_ref, near.at[1, 1], 9, left),
        over_band(f_ref, near.at[1, 0], 7, left),
    ]
    for a, b in zip(to_right, to_left):
        a.start()
        b.start()
    say(0)
    wide[0] = w_ref[...]
    near[0, 0] = f_ref[...]
    near[0, 1] = b_ref[...]
    hear(0)
    say(1)
    own = []
    for r in range(4):
        both = []
        for src in (f_ref, b_ref):
            rows = src[r * bands : (r + 1) * bands, :]
            both += [rows, jnp.concatenate([rows[:, half:], -rows[:, :half]], 1)]
        own.append(halves(jnp.concatenate(both, 0)))

    def margin_of(slot):
        total = None
        for r in range(4):
            term = triple(own[r], halves(wide[slot, r * bands : (r + 1) * bands, :]), NT)
            total = term if total is None else total + term
        nmat[0, :, slot * bands : (slot + 1) * bands] = total

    hear(1)
    say(2)
    to_right[0].wait_recv()
    far_right = over_band(wide.at[3, lower], wide.at[2, lower], 4, right)
    far_right.start()
    to_left[0].wait_recv()
    far_left = over_band(wide.at[1, upper], wide.at[2, upper], 5, left)
    far_left.start()
    hear(2)
    for k in range(3, rounds - 1):
        learn(k)
    if rounds > 3:
        say(rounds - 1)
    margin_of(0)
    to_right[1].wait_recv()
    margin_of(3)
    to_left[1].wait_recv()
    margin_of(1)
    far_right.wait_recv()
    far_left.wait_recv()
    margin_of(2)
    turned = pltpu.roll(nmat[0], mx * bands, 1)
    mpart[...] = turned.reshape(mpart.shape)
    if rounds > 3:
        hear(rounds - 1)
    say_to_partner()

    to_partner(mpart, mpair, mm).start()
    to_owners(mpart, mpair, msum, mrs, mm)
    for r in range(4):
        for part in range(2):
            rows = slice(r * every, (r + 1) * every)
            lanes = slice(part * half, (part + 1) * half)
            ph_ref[rows, lanes], pl_ref[rows, lanes] = halves(p_ref[:, part, r, :])
    u = me * 4 + iota((4 * bands, half), 0) // bands
    w = iota((4 * bands, half), 1)
    u, w = centred(u, 4 * n), centred(w, half)
    diag_ref[...] = kinetic_scale * (u * u + w * w) + shift_ref[...]
    columns = jnp.concatenate([pot_ref[...]] * 2, 0).T
    at = iota((4 * n, LANES), 1) // bands
    spread = jnp.zeros((4 * n, LANES), jnp.float32)
    for k in range(4):
        spread = jnp.where(at == k, columns[:, k : k + 1], spread)
    pots_ref[...] = spread
    shape = t2h_ref.shape
    row_part, lane_part = iota(shape, 0) % TILE // (TILE // 2), iota(shape, 1) // half
    flip = jnp.where(row_part == lane_part, 1.0, -1.0)
    inverse_table = (t2h_ref[...].astype(jnp.float32) + t2l_ref[...].astype(jnp.float32)) * flip
    t3h_ref[...], t3l_ref[...] = halves(inverse_table)
    t1h_ref[...], t1l_ref[...] = halves(inverse_table.T)
    owners_tell(mrs, mfull, mm)
    to_right[2].wait_recv()
    far_f = over_band(near.at[3, 0], near.at[2, 0], 10, right)
    far_f.start()
    to_left[2].wait_recv()
    far_b = over_band(near.at[1, 1], near.at[2, 1], 11, left)
    far_b.start()
    told(mfull, mm)
    mine_half = pl.ds(core * (mfull.shape[0] // 2), mfull.shape[0] // 2)
    mall[pl.ds(mx, 1)] = mfull[mine_half][None]
    for step in range(1, nx):
        t = lax.rem(mx + step, nx)
        remote(mfull.at[mine_half], mall.at[mx], ms, mr, "band", t).start()
    some = mall.at[pl.ds(0, nx - 1)]
    across = remote(some, some, ms, mr, "band", right)
    across.wait_recv()

    def margin_full(part):
        tiles_each = bands // TILE
        at = slice(part * tiles_each, (part + 1) * tiles_each)
        rows = [mall[x, at].reshape(bands, every) for x in range(nx)]
        return jnp.concatenate(rows, 0) / points

    real, imag = margin_full(0), margin_full(1)
    nmat[0] = exact(real, real, NT) + exact(imag, imag, NT)
    nmat[1] = exact(imag, real, NT) - exact(real, imag, NT)
    qt[0] = real.T
    qt[1] = imag.T

    def times(a, b):
        return a[0] * b[0] - a[1] * b[1], a[0] * b[1] + a[1] * b[0]

    def minus(a, b):
        return a[0] - b[0], a[1] - b[1]

    def conj(a):
        return a[0], -a[1]

    def solver(first, last, across):
        scale = 1.0 / (first * last - across[0] * across[0] - across[1] * across[1])
        first, last = first * scale, last * scale
        across = (across[0] * scale, across[1] * scale)

        def solve(x, y):
            new_x = minus((last * x[0], last * x[1]), times(across, y))
            return new_x, minus((first * y[0], first * y[1]), times(conj(across), x))

        return solve

    def eliminate(step, carry):
        c = 4 * step
        lane = iota((every, every), 1)
        at_0 = jnp.full((every, every), 0, jnp.int32) + c
        line = iota((1, every), 1)
        lows, highs = (line == c) | (line == c + 1), (line == c + 2) | (line == c + 3)
        on = (lane >= c) & (lane < c + 4)

        def without(row, where):
            return jnp.where(where, 0.0, row[0]), jnp.where(where, 0.0, row[1])

        def unit(row, where, k):
            return jnp.where(where, jnp.where(line == c + k, 1.0, 0.0), row[0]), jnp.where(where, 0.0, row[1])

        real, imag = nmat[0], nmat[1]
        rows = [
            (nmat[0, pl.ds(c + k, 1), :], nmat[1, pl.ds(c + k, 1), :])
            for k in range(4)
        ]

        def one(row, k):
            return jnp.sum(jnp.where(line == c + k, row, 0.0), axis=1, keepdims=True)

        def element(j, k):
            return one(rows[j][0], k), one(rows[j][1], k)

        diag4 = [one(rows[k][0], k) for k in range(4)]
        off = {(j, k): element(j, k) for j in range(4) for k in range(j + 1, 4)}
        solve = solver(diag4[0], diag4[1], off[0, 1])
        head = {k: solve(off[0, k], off[1, k]) for k in (2, 3)}

        def rest(j, k, value):
            value = minus(value, times(conj(off[0, j]), head[k][0]))
            return minus(value, times(conj(off[1, j]), head[k][1]))

        zero = jnp.zeros_like(diag4[2])
        last_solve = solver(
            rest(2, 2, (diag4[2], zero))[0], rest(3, 3, (diag4[3], zero))[0], rest(2, 3, off[2, 3])
        )
        new = list(solve(unit(rows[0], lows, 0), unit(rows[1], lows, 1)))
        tail = []
        for k in (2, 3):
            row = minus(without(rows[k], lows), times(conj(off[0, k]), new[0]))
            row = minus(row, times(conj(off[1, k]), new[1]))
            tail.append(unit(row, highs, k))
        tail = last_solve(*tail)
        for k in range(2):
            row = minus(without(new[k], highs), times(head[2][k], tail[0]))
            new[k] = minus(row, times(head[3][k], tail[1]))
        new += tail
        total = jnp.where(on, 0.0, real), jnp.where(on, 0.0, imag)
        for k in range(4):
            column = (
                jnp.take_along_axis(real, at_0 + k, axis=1),
                jnp.take_along_axis(imag, at_0 + k, axis=1),
            )
            total = minus(total, times(column, new[k]))
        nmat[0], nmat[1] = total
        for k in range(4):
            nmat[0, pl.ds(c + k, 1), :] = new[k][0]
            nmat[1, pl.ds(c + k, 1), :] = new[k][1]
        return carry

    lax.fori_loop(0, every // 4, eliminate, 0)

    mine = pl.ds(pl.multiple_of(mx * bands, TILE), bands)
    qr, qi = qt[0, mine, :], qt[1, mine, :]
    nr, ni = nmat[0], nmat[1]
    zr = exact(qr, nr) + exact(qi, ni)
    zi = exact(qr, ni) - exact(qi, nr)
    both = pltpu.roll(jnp.concatenate([zr, zi], 0), lax.rem((nx - mx) * bands, every), 1)
    zmat[pl.ds(core, 1)] = jnp.where(core == 0, both, -both)[None]
    swap = remote(zmat.at[core], zmat.at[core], zs, zr_sem, "pw", partner)
    swap.start()

    to_right[3].wait_recv()
    to_left[3].wait_recv()
    far_f.wait_recv()
    far_b.wait_recv()
    hear_partner()
    swap.wait_recv()
    coeff = jnp.concatenate([zmat[0], zmat[1]], 1)
    for r in range(4):
        rows = slice(r * bands, (r + 1) * bands)
        blocks = [near[d, which, rows, :] for which in range(2) for d in range(nx)]
        mixed = exact(coeff, jnp.concatenate(blocks, 0))
        dr = (mixed[:bands, :half] - mixed[bands:, half:]) / (2.0 * string_step)
        di = (mixed[:bands, half:] + mixed[bands:, :half]) / (2.0 * string_step)
        der_raw[:, 0, r, :] = dr
        der_raw[:, 1, r, :] = di
        vec[rows, :half] = -dr
        vec[rows, half:] = -di

    def half_way(src, send):
        parts = halves(src[...])
        out = triple((t2h_ref[...], t2l_ref[...]), parts, NT)
        send[...] = swap_blocks(out.reshape(n, TILE, LANES))

    def fields(recv, sem):
        arrived(recv, n - 1, er.at[sem])
        parts = halves(recv[...].reshape(n * TILE, LANES))
        return triple((t1h_ref[...], t1l_ref[...]), parts)

    def project(src, part, pair, sem):
        total = None
        for r in range(4):
            rows = src[r * bands : (r + 1) * bands, :]
            both = jnp.concatenate([rows, jnp.concatenate([rows[:, half:], -rows[:, :half]], 1)], 0)
            at = slice(r * every, (r + 1) * every)
            term = triple(halves(both), (ph_ref[at, :], pl_ref[at, :]), NT)
            total = term if total is None else total + term
        part[...] = (total / points).reshape(part.shape)
        to_partner(part, pair, sem).start()

    def per_band(values):
        return sum(values[r * bands : (r + 1) * bands] for r in range(1, 4)) + values[:bands]

    def summed(values):
        return per_band(jnp.sum(values, axis=1, keepdims=True))

    def as_row(column, first):
        shape = (column.shape[0], LANES)
        chosen = iota(shape, 1) == iota(shape, 0) + first
        return jnp.sum(jnp.where(chosen, column, 0.0), axis=0, keepdims=True)

    def as_column(row, first):
        shape = (bands, LANES)
        chosen = iota(shape, 1) == iota(shape, 0) + first
        return jnp.sum(jnp.where(chosen, row, 0.0), axis=1, keepdims=True)

    def lanes_per_band(row, first):
        row = row + pltpu.roll(row, LANES // 2, 1)
        row = row + pltpu.roll(row, LANES // 4, 1)
        lane = iota(row.shape, 1)
        return jnp.where((lane >= first) & (lane < first + bands), row, 0.0)

    def down_rows(column):
        return jnp.concatenate([column] * 4, 0)

    diag = jnp.concatenate([diag_ref[...]] * 2, 1)
    stren = str_ref[...]

    project(vec, cpart, cpair, cm)
    half_way(vec, sendb)
    to_owners(cpart, cpair, csum, crs, cm)
    exchange(sendb, recvb, es.at[0], er.at[0])
    d = vec[...]
    scal_row = as_row(summed(diag * d * d), 0) + as_row(summed(d * d), 2 * bands)
    owners_tell(crs, cfull, cm)
    field = fields(recvb, 0)
    field_ref[...] = field
    pot = jnp.concatenate([pots_ref[...]] * 2, 0)
    weighted = field * pot
    energy = jnp.sum(weighted * field, axis=0, keepdims=True)
    sendc[...] = triple((t3h_ref[...], t3l_ref[...]), halves(weighted)).reshape(sendc.shape)
    exchange(sendc, recvc, es.at[1], er.at[1])
    scal[0] = scal_row + lanes_per_band(energy, 0)
    add_up(scal, spair, scals, sm)

    told(cfull, cm)
    told_chip(cfull, cm)
    coupled = cfull[...].reshape(2 * bands, every)
    weights = halves(coupled * stren)
    for r in range(4):
        at = slice(r * every, (r + 1) * every)
        rows = slice(r * bands, (r + 1) * bands)
        mixed = triple(weights, (ph_ref[at, :], pl_ref[at, :]))
        img[rows, :half] = mixed[:bands, :half] - mixed[bands:, half:]
        img[rows, half:] = mixed[:bands, half:] + mixed[bands:, :half]
    pair = jnp.sum(stren * coupled * coupled, axis=1, keepdims=True)
    own_pair = points * (pair[:bands] + pair[bands:])
    totals = added_up(scals, sm)
    norm_now = as_column(totals, 2 * bands)
    curvature = as_column(totals, 0) + own_pair
    alpha = norm_now / curvature

    arrived(recvc, n - 1, er.at[1])
    back = swap_blocks(recvc[...]).reshape(n * TILE, LANES).T
    smooth = triple(halves(back), (t2h_ref[...], t2l_ref[...]))
    d = vec[...]
    image = diag * d + smooth + img[...]
    res[...] = d - down_rows(alpha) * image

    project(res, cpart2, cpair2, cm2)
    half_way(res, sende)
    to_owners(cpart2, cpair2, csum2, crs2, cm2)
    exchange(sende, recve, es.at[2], er.at[2])
    d, r2 = vec[...], res[...]
    stiff = diag * r2
    row2 = as_row(summed(stiff * r2), 0) + as_row(summed(stiff * d), bands)
    row2 = row2 + as_row(summed(r2 * r2), 2 * bands)
    scal2[0] = row2
    owns2, tile2 = owner_of(cpart2.shape[0])

    @pl.when(owns2)
    def _():
        arrived(crs2, chips - 1, cm2.at[3])
        t = tile2
        mine = jnp.sum(crs2[...], axis=0)
        old = cfull[pl.ds(t, 1)].reshape(TILE, every)
        first = lax.rem(t * TILE, bands)
        with_mine = points * jnp.sum(stren * mine * mine, axis=1, keepdims=True)
        with_old = points * jnp.sum(stren * mine * old, axis=1, keepdims=True)
        scal2[0] = scal2[0] + as_row(with_mine, first) + as_row(with_old, first + bands)

    field2 = fields(recve, 2)
    weighted2 = field2 * jnp.concatenate([pots_ref[...]] * 2, 0)
    own2 = jnp.sum(weighted2 * field2, axis=0, keepdims=True)
    cross2 = jnp.sum(weighted2 * field_ref[...], axis=0, keepdims=True)
    scal2[0] = scal2[0] + lanes_per_band(own2, 0) + lanes_per_band(cross2, bands)
    add_up(scal2, spair2, scals2, sm2)
    totals2 = added_up(scals2, sm2)
    norm_next = as_column(totals2, 2 * bands)
    beta = norm_next / norm_now
    curvature2 = (
        as_column(totals2, 0) + 2.0 * beta * as_column(totals2, bands) + beta * beta * curvature
    )
    alpha2 = norm_next / curvature2
    of_first = alpha + alpha2 * beta
    for r in range(4):
        rows = slice(r * bands, (r + 1) * bands)
        total = of_first * vec[rows, :] + alpha2 * res[rows, :]
        for part in range(2):
            sol_raw[:, part, r, :] = total[:, part * half : (part + 1) * half]

    for copy in to_right + to_left + [far_right, far_left, far_f, far_b]:
        copy.wait_send()
    across.wait_send()
    swap.wait_send()
    sent_to_owners(mpart, msum, mm)
    owners_done(mrs, mfull, mm)
    sent_to_owners(cpart, csum, cm)
    owners_done(crs, cfull, cm)
    left_here(cfull, cfull.shape[0] // 2, cm.at[6])
    sent_to_owners(cpart2, csum2, cm2)
    left_here(sendb, n - 1, es.at[0])
    left_here(sendc, n - 1, es.at[1])
    left_here(sende, n - 1, es.at[2])
    adding_done(scal, scals, sm)
    adding_done(scal2, scals2, sm2)


def centred(index, length):
    shifted = (index + length // 2) % length - length // 2
    return shifted.astype(jnp.float32) / length


def split_table(table):
    table = table.astype(np.float32)
    high = table.astype(ml_dtypes.bfloat16)
    low = (table - high.astype(np.float32)).astype(ml_dtypes.bfloat16)
    return high, low


def tables(length, peers):
    index = np.arange(length)
    angle = (index[:, None] * index[None, :] % length) * (2.0 * math.pi / length)
    cosine, sine = np.cos(angle) / math.sqrt(length), np.sin(angle) / math.sqrt(length)
    out = np.block([[cosine, -sine], [sine, cosine]])
    order = np.arange(2 * length).reshape(2, peers, length // peers).transpose(1, 0, 2).reshape(-1)
    return split_table(out[order])


def body(n, nx, waves, forward, backward, projectors, potential, strengths, shifts):
    bands, parts, rows, width = waves.shape
    length = rows * n
    points = float(length * width)
    every = nx * bands
    count = projectors.shape[0]
    shape = (rows * bands, parts * width)
    f32 = functools.partial(pltpu.VMEM, dtype=jnp.float32)
    full, line, tiles = (n, TILE, LANES), (n // 2, TILE, LANES), 2 * bands // TILE
    vmem = pl.BlockSpec(memory_space=pltpu.VMEM)
    dma = pltpu.SemaphoreType.DMA
    der, sol = pl.pallas_call(
        functools.partial(kernel, n, nx, points),
        out_shape=[jax.ShapeDtypeStruct(waves.shape, jnp.float32)] * 2,
        in_specs=[vmem] * 9,
        out_specs=[vmem] * 2,
        scratch_shapes=[
            f32(shape), f32(shape), f32(shape),
            f32((rows * bands, width)), f32((length, LANES)),
            *[pltpu.VMEM((rows * count, parts * width), jnp.bfloat16)] * 2,
            *[pltpu.VMEM((2 * length, 2 * length), jnp.bfloat16)] * 4,
            f32((nx, *shape)), f32((2, every, every)),
            f32((nx, 2, *shape)),
            f32((2 * tiles, TILE, LANES)), *[f32((tiles, TILE, LANES))] * 2, f32(line),
            f32((2 * tiles, TILE, LANES)),
            f32((nx, tiles, TILE, LANES)), f32((2, every, every)), f32((2, 2 * bands, every)),
            f32(shape), f32(shape), f32(shape),
            f32(full), f32(full), f32(full), f32(full), f32(full), f32(full),
            f32((tiles, TILE, LANES)), *[f32((tiles // 2, TILE, LANES))] * 2, f32(line),
            f32((tiles, TILE, LANES)),
            f32((tiles, TILE, LANES)), *[f32((tiles // 2, TILE, LANES))] * 2, f32(line),
            *[f32((2, 1, LANES)), f32((1, LANES)), f32((n // 2, 1, LANES))] * 2,
            f32((n * TILE, LANES)),
            pltpu.SemaphoreType.REGULAR((n.bit_length(),)),
            dma((12,)), dma((12,)), dma, dma, dma, dma, dma((8,)), dma((8,)), dma((8,)), dma((4,)), dma((4,)),
            dma((3,)), dma((3,)),
        ],
        compiler_params=pltpu.CompilerParams(
            collective_id=0, has_side_effects=True, vmem_limit_bytes=60 * 1024 * 1024
        ),
    )(
        waves, forward, backward, projectors, jnp.tile(shifts, rows).reshape(-1, 1), potential,
        strengths.reshape(1, count), *[jnp.asarray(t) for t in tables(length, n)],
    )

    return sol, der


def solution(mesh):
    bands = P("band", "kgrp", "pw", None)
    return jax.shard_map(
        functools.partial(body, mesh.shape["pw"], mesh.shape["band"]),
        mesh=mesh,
        in_specs=(bands, bands, bands, P("kgrp", None, "pw", None), P("pw", None), P(), P("band")),
        out_specs=(bands, bands),
        check_vma=False,
    )
```
